8 devices in a mesh: dp: 1 (over z), tp: 8 (over y, x, core).
Axes of the slice: x: 2, y: 2, z: 1, core: 2. Of those that a mesh axis runs over, the one named last changes fastest.
Arguments:
- hidden: bfloat16 [1, 4096, 5120], P('dp', 'tp')
- attn_gain: float32 [5120], replicated
- w_q: bfloat16 [5120, 5120], P(None, 'tp')
- w_k: bfloat16 [5120, 5120], P(None, 'tp')
- w_v: bfloat16 [5120, 5120], P(None, 'tp')
- q_gain: float32 [5120], P('tp')
- k_gain: float32 [5120], P('tp')
- w_o: bfloat16 [5120, 5120], P('tp')
Outputs:
- output 1: bfloat16 [1, 4096, 5120], P('dp', 'tp')
- output 2: bfloat16 [1, 4096, 40, 128], P('dp', None, 'tp')
- output 3: bfloat16 [1, 4096, 40, 128], P('dp', None, 'tp')
All inputs are finite; a program needn't handle non-finite values.
Results may differ from the reference program's by a relative error of at most 0.00944418.
Values are sent between devices in bfloat16 or wider.
A program may use at most 1 GiB of HBM per device.

```python
import jax
import jax.numpy as jnp
from jax import lax

BATCH_SIZE = 1
SEQ_LEN = 4096
D_MODEL = 5120
N_HEADS = 40
HEAD_DIM = 128


def setup_inputs(seed: int = 0, part: int = 0) -> dict:
    base_key = jax.random.key(seed)
    part_keys = jax.random.split(jax.random.fold_in(base_key, part), 2)
    key_list = jax.random.split(base_key, 9)
    x_noise = jax.random.normal(part_keys[0], (BATCH_SIZE, SEQ_LEN, D_MODEL), jnp.float32)
    x_mean = jax.random.normal(part_keys[1], (BATCH_SIZE, 1, D_MODEL), jnp.float32)
    head_pos = jnp.arange(N_HEADS, dtype=jnp.float32) / max(N_HEADS - 1, 1)
    q_heads = 10.0 ** (head_pos - 0.5) * jax.random.uniform(key_list[0], (N_HEADS,), jnp.float32, 0.8, 1.2)
    k_heads = 10.0 ** (0.5 - head_pos) * jax.random.uniform(key_list[1], (N_HEADS,), jnp.float32, 0.8, 1.2)
    fan_scale = D_MODEL ** -0.5
    w_shape = (D_MODEL, D_MODEL)
    w_q = jax.random.normal(key_list[2], w_shape, jnp.float32) * (fan_scale * jnp.repeat(q_heads, HEAD_DIM))[None, :]
    w_k = jax.random.normal(key_list[3], w_shape, jnp.float32) * (fan_scale * jnp.repeat(k_heads, HEAD_DIM))[None, :]
    w_v = jax.random.normal(key_list[4], w_shape, jnp.float32) * fan_scale
    w_o = jax.random.normal(key_list[5], w_shape, jnp.float32) * fan_scale
    return {
        'hidden': (x_noise + x_mean).astype(jnp.bfloat16),
        'attn_gain': jax.random.uniform(key_list[6], (D_MODEL,), jnp.float32, 0.5, 1.5),
        'w_q': w_q.astype(jnp.bfloat16),
        'w_k': w_k.astype(jnp.bfloat16),
        'w_v': w_v.astype(jnp.bfloat16),
        'q_gain': jax.random.uniform(key_list[7], (D_MODEL,), jnp.float32, 1.5, 3.5),
        'k_gain': jax.random.uniform(key_list[8], (D_MODEL,), jnp.float32, 1.5, 3.5),
        'w_o': w_o.astype(jnp.bfloat16),
    }


def rope_tables(seq_len, head_dim):
    half_dim = head_dim // 2
    inv_freq = 10000.0 ** (-jnp.arange(half_dim, dtype=jnp.float32) * (2.0 / head_dim))
    angles = jnp.arange(seq_len, dtype=jnp.float32)[:, None] * inv_freq[None, :]
    return jnp.cos(angles), jnp.sin(angles)


def apply_rope(heads_in, cos_tab, sin_tab):
    half_dim = heads_in.shape[-1] // 2
    lower_half = heads_in[..., :half_dim]
    upper_half = heads_in[..., half_dim:]
    cos_bcast = cos_tab[None, :, None, :]
    sin_bcast = sin_tab[None, :, None, :]
    return jnp.concatenate([lower_half * cos_bcast - upper_half * sin_bcast, upper_half * cos_bcast + lower_half * sin_bcast], axis=-1)


def reference(hidden, attn_gain, w_q, w_k, w_v, q_gain, k_gain, w_o):
    x_f32 = hidden.astype(jnp.float32)
    inv_rms = lax.rsqrt(jnp.mean(x_f32 * x_f32, axis=-1, keepdims=True) + 1e-5)
    h_rows = (x_f32 * inv_rms * attn_gain).astype(jnp.bfloat16).reshape(BATCH_SIZE * SEQ_LEN, D_MODEL)
    q_raw = jnp.dot(h_rows, w_q, preferred_element_type=jnp.float32).astype(jnp.bfloat16).astype(jnp.float32)
    k_raw = jnp.dot(h_rows, w_k, preferred_element_type=jnp.float32).astype(jnp.bfloat16).astype(jnp.float32)
    v_rows = jnp.dot(h_rows, w_v, preferred_element_type=jnp.float32).astype(jnp.bfloat16)
    q_normed = q_raw * lax.rsqrt(jnp.mean(q_raw * q_raw, axis=-1, keepdims=True) + 1e-5) * q_gain
    k_normed = k_raw * lax.rsqrt(jnp.mean(k_raw * k_raw, axis=-1, keepdims=True) + 1e-5) * k_gain
    cos_tab, sin_tab = rope_tables(SEQ_LEN, HEAD_DIM)
    head_shape = (BATCH_SIZE, SEQ_LEN, N_HEADS, HEAD_DIM)
    q_rot = apply_rope(q_normed.reshape(head_shape), cos_tab, sin_tab).astype(jnp.bfloat16)
    k_rot = apply_rope(k_normed.reshape(head_shape), cos_tab, sin_tab).astype(jnp.bfloat16)
    v_heads = v_rows.reshape(head_shape)
    positions = jnp.arange(SEQ_LEN)
    causal = positions[:, None] >= positions[None, :]
    score_scale = HEAD_DIM ** -0.5

    def one_head(head_args):
        q_head, k_head, v_head = head_args
        scores = jnp.einsum('bqd,bkd->bqk', q_head.astype(jnp.float32), k_head.astype(jnp.float32)) * score_scale
        scores = jnp.where(causal[None], scores, -1e30)
        prob_bf = jax.nn.softmax(scores, axis=-1).astype(jnp.bfloat16)
        head_out = jnp.einsum('bqk,bkd->bqd', prob_bf.astype(jnp.float32), v_head.astype(jnp.float32))
        return head_out.astype(jnp.bfloat16)

    per_head = lax.map(one_head, (jnp.moveaxis(q_rot, 2, 0), jnp.moveaxis(k_rot, 2, 0), jnp.moveaxis(v_heads, 2, 0)))
    attn_rows = jnp.moveaxis(per_head, 0, 2).reshape(BATCH_SIZE * SEQ_LEN, D_MODEL)
    y_rows = jnp.dot(attn_rows, w_o, preferred_element_type=jnp.float32).astype(jnp.bfloat16)
    hidden_out = (x_f32 + y_rows.reshape(hidden.shape).astype(jnp.float32)).astype(jnp.bfloat16)
    return (hidden_out, k_rot, v_heads)
```

```python
import functools

import jax
import jax.numpy as jnp
import numpy as np
from jax import lax
from jax.experimental import pallas as pl
from jax.experimental.pallas import tpu as pltpu
from jax.sharding import PartitionSpec as P

MESH = pl.DeviceIdType.MESH
HEAD_DIM = 128
HEADS = 5
COLS = HEADS * HEAD_DIM
WIDTH = 5120
BLOCK = 512
TP = 8
SEQ = TP * BLOCK
PIECES = 4
PIECE = BLOCK // PIECES
UNIT = 256
STEPS = 8
ROWS = BLOCK // STEPS
HALF = WIDTH // 2
TILE = 512
F32 = jnp.float32
BF16 = jnp.bfloat16
SIB, XN, YN, DG, SX, SY, SDG = range(7)


class Place:
    def __init__(self):
        me = lax.axis_index("tp")
        self.dp = lax.axis_index("dp")
        self.me = me
        self.core = me % 2
        self.x = (me // 2) % 2
        self.y = me // 4

    def at(self, fx, fy, fc):
        x = self.x + fx * (1 - 2 * self.x)
        y = self.y + fy * (1 - 2 * self.y)
        c = self.core + fc * (1 - 2 * self.core)
        return (y * 2 + x) * 2 + c

    def kind(self, k):
        fx, fy, fc = ((0, 0, 1), (1, 0, 0), (0, 1, 0), (1, 1, 0), (1, 0, 1), (0, 1, 1), (1, 1, 1))[k]
        return self.at(fx, fy, fc)

    def dev(self, index):
        return (self.dp, index)


def barrier_with(place, kinds):
    sem = pltpu.get_barrier_semaphore()
    for k in kinds:
        pl.semaphore_signal(sem, inc=1, device_id=place.dev(place.kind(k)), device_id_type=MESH)
    pl.semaphore_wait(sem, len(kinds))


def diagonal():
    r = lax.broadcasted_iota(jnp.int32, (128, 128), 0)
    c = lax.broadcasted_iota(jnp.int32, (128, 128), 1)
    return r == c


def gather_project(h_ref, wq_ref, wk_ref, wv_ref, qkv_ref, ssq_ref, hbuf,
                   w_v, h_v, st, ssq_v, w_sem, h_sem, o_sem, send_sem, recv_sem, ss_send, ss_recv, ss_loc):
    place = Place()
    for n, w in enumerate((wq_ref, wk_ref, wv_ref)):
        pltpu.make_async_copy(w, w_v.at[n], w_sem.at[n]).start()
    barrier_with(place, range(7))

    def copy(src_ref, block, p, send, kind, target):
        return pltpu.make_async_remote_copy(
            src_ref=src_ref, dst_ref=hbuf.at[block, pl.ds(p * PIECE, PIECE)],
            send_sem=send_sem.at[send, p], recv_sem=recv_sem.at[kind, p],
            device_id=place.dev(place.kind(target)), device_id_type=MESH)

    def own(p, send, kind):
        return copy(h_ref.at[pl.ds(p * PIECE, PIECE)], place.me, p, send, kind, kind)

    def relay(owner, p, send, kind, target):
        block = place.kind(owner)
        return copy(hbuf.at[block, pl.ds(p * PIECE, PIECE)], block, p, send, kind, target)

    def arrived(kind, p):
        relay(kind, p, 0, kind, SIB).wait_recv()

    for p in range(PIECES):
        own(p, 0, XN).start()
        own(p, 1, YN).start()
        own(p, 2, SIB).start()

    def forwards(p):
        out = [(XN, p, 3, SX, SIB), (YN, p, 4, SY, SIB)]
        out.append((XN, p, 5, DG, YN) if p % 2 == 0 else (YN, p, 5, DG, XN))
        return out

    def unit(u):
        a = u // 4
        v = u - 4
        w = v % 4
        z = u - 12
        near = a == 0
        far = a == 3
        fc = jnp.where(near, u // 2, jnp.where(far, z % 2, w // 2))
        half = jnp.where(near, u % 2, jnp.where(far, z // 2, v // 4))
        fy = jnp.where(near, 0, jnp.where(far, 1, w % 2))
        fx = jnp.where(near, 0, jnp.where(far, 1, 1 - w % 2))
        return place.at(fx, fy, fc), half

    def load(u, slot, own_rows):
        block, half = unit(u)
        rows = pl.ds(pl.multiple_of(half * UNIT, UNIT), UNIT)
        if own_rows:
            return pltpu.make_async_copy(h_ref.at[rows], h_v.at[slot], h_sem.at[slot])
        return pltpu.make_async_copy(hbuf.at[block, rows], h_v.at[slot], h_sem.at[slot])

    def start_load(u):
        @pl.when(u < 2)
        def _():
            load(u, u % 2, True).start()

        @pl.when(u >= 2)
        def _():
            load(u, u % 2, False).start()

    def store(u, slot):
        block, half = unit(u)
        rows = pl.ds(pl.multiple_of(block * BLOCK + half * UNIT, UNIT), UNIT)
        return pltpu.make_async_copy(st.at[slot], qkv_ref.at[:, :, rows, :], o_sem.at[slot])

    eye = diagonal()

    def step(u, carry):
        slot = u % 2
        for first, p0 in ((4, 0), (8, 2)):
            @pl.when(u == first)
            def _(p0=p0):
                for p in (p0, p0 + 1):
                    arrived(XN, p)
                    arrived(YN, p)
                    for f in forwards(p):
                        relay(*f).start()
        for first, p0 in ((12, 0), (14, 2)):
            @pl.when(u == first)
            def _(p0=p0):
                for p in (p0, p0 + 1):
                    arrived(DG, p)
                    relay(DG, p, 6, SDG, SIB).start()

        @pl.when((u % 4 == 0) | (u == 14))
        def _():
            start_load(u)

        for nxt, kind, p0 in ((2, SIB, 0), (3, SIB, 2), (6, SX, 0), (7, SY, 0), (10, SX, 2), (11, SY, 2), (13, SDG, 0), (15, SDG, 2)):
            @pl.when(u + 1 == nxt)
            def _(kind=kind, p0=p0):
                arrived(kind, p0)
                arrived(kind, p0 + 1)

        @pl.when(((u + 1) % 4 != 0) & (u + 1 != 14))
        def _():
            start_load(u + 1)

        @pl.when(u == 0)
        def _():
            for n, w in enumerate((wq_ref, wk_ref, wv_ref)):
                pltpu.make_async_copy(w, w_v.at[n], w_sem.at[n]).wait()

        load(u, slot, False).wait()

        @pl.when(u >= 2)
        def _():
            store(u - 2, slot).wait()

        block, half = unit(u)

        def part(n, c):
            r = jnp.dot(h_v[slot], w_v[n], preferred_element_type=F32).astype(BF16)
            for h in range(HEADS):
                st[slot, n, h] = r[:, h * HEAD_DIM:(h + 1) * HEAD_DIM]

            @pl.when(n < 2)
            def _():
                rf = r.astype(F32)
                col = jnp.sum(rf * rf, axis=1, keepdims=True)
                for b in range(UNIT // 128):
                    row = jnp.sum(jnp.where(eye, col[b * 128:(b + 1) * 128], 0.0), axis=0, keepdims=True)
                    ssq_v[pl.ds(block * 8 + n * 4 + half * 2 + b, 1), :] = row
            return c

        lax.fori_loop(0, 3, part, 0)
        store(u, slot).start()
        return carry

    lax.fori_loop(0, 16, step, 0)

    def share(k):
        return pltpu.make_async_remote_copy(
            src_ref=ssq_v, dst_ref=ssq_ref.at[place.me], send_sem=ss_send.at[k], recv_sem=ss_recv.at[k],
            device_id=place.dev(place.kind(k)), device_id_type=MESH)

    def shared(k):
        return pltpu.make_async_remote_copy(
            src_ref=ssq_v, dst_ref=ssq_ref.at[place.kind(k)], send_sem=ss_send.at[k], recv_sem=ss_recv.at[k],
            device_id=place.dev(place.kind(k)), device_id_type=MESH)

    for k in range(7):
        share(k).start()
    mine = pltpu.make_async_copy(ssq_v, ssq_ref.at[place.me], ss_loc)
    mine.start()
    store(14, 0).wait()
    store(15, 1).wait()
    for p in range(PIECES):
        own(p, 0, XN).wait_send()
        own(p, 1, YN).wait_send()
        own(p, 2, SIB).wait_send()
        for f in forwards(p):
            relay(*f).wait_send()
        relay(DG, p, 6, SDG, SIB).wait_send()
    mine.wait()
    for k in range(7):
        share(k).wait_send()
        shared(k).wait_recv()


def gather_project_call(h, wq, wk, wv):
    any_spec = pl.BlockSpec(memory_space=pl.ANY)
    return pl.pallas_call(
        gather_project,
        out_shape=[jax.ShapeDtypeStruct((3, HEADS, SEQ, HEAD_DIM), BF16),
                   jax.ShapeDtypeStruct((TP, 64, 128), F32),
                   jax.ShapeDtypeStruct((TP, BLOCK, WIDTH), BF16)],
        in_specs=[any_spec] * 4,
        out_specs=[any_spec] * 3,
        scratch_shapes=[
            pltpu.VMEM((3, WIDTH, COLS), BF16),
            pltpu.VMEM((2, UNIT, WIDTH), BF16),
            pltpu.VMEM((2, 3, HEADS, UNIT, HEAD_DIM), BF16),
            pltpu.VMEM((64, 128), F32),
            pltpu.SemaphoreType.DMA((3,)),
            pltpu.SemaphoreType.DMA((2,)),
            pltpu.SemaphoreType.DMA((2,)),
            pltpu.SemaphoreType.DMA((7, PIECES)),
            pltpu.SemaphoreType.DMA((7, PIECES)),
            pltpu.SemaphoreType.DMA((7,)),
            pltpu.SemaphoreType.DMA((7,)),
            pltpu.SemaphoreType.DMA(()),
        ],
        compiler_params=pltpu.CompilerParams(collective_id=0, has_side_effects=True, vmem_limit_bytes=60 * 2**20),
        name="gather_project",
    )(h, wq, wk, wv)


def rotate_heads(qk_ref, ssq_ref, gain_ref, tab_ref, q_ref, k_ref):
    eye = diagonal()
    total = jnp.sum(ssq_ref[...], axis=0)
    low = lax.broadcasted_iota(jnp.int32, (128, 128), 1) < 64
    for b in range(BLOCK // 128):
        rows = slice(b * 128, (b + 1) * 128)
        t = tab_ref[rows, :]
        turned = pltpu.roll(t, 64, 1)
        cos = jnp.where(low, t, turned)
        sin = jnp.where(low, -turned, t)
        for n in range(2):
            col = jnp.sum(jnp.where(eye, total[n * 4 + b:n * 4 + b + 1], 0.0), axis=1, keepdims=True)
            inv = lax.rsqrt(col / WIDTH + 1e-5)
            for h in range(HEADS):
                x = qk_ref[n, h, rows, :].astype(F32) * inv * gain_ref[n, h:h + 1, :]
                r = (x * cos + pltpu.roll(x, 64, 1) * sin).astype(BF16)
                if n == 0:
                    for g in range(128 // ROWS):
                        q_ref[h, b * (128 // ROWS) + g, 0] = r[g * ROWS:(g + 1) * ROWS]
                else:
                    k_ref[h, rows, :] = r


def rotate_heads_call(qkv, ssq, gains, table):
    return pl.pallas_call(
        rotate_heads,
        grid=(TP,),
        out_shape=[jax.ShapeDtypeStruct((HEADS, STEPS, TP, ROWS, HEAD_DIM), BF16),
                   jax.ShapeDtypeStruct((HEADS, SEQ, HEAD_DIM), BF16)],
        in_specs=[pl.BlockSpec((2, HEADS, BLOCK, HEAD_DIM), lambda i: (0, 0, i, 0)),
                  pl.BlockSpec((TP, 8, 128), lambda i: (0, i, 0)),
                  pl.BlockSpec((2, HEADS, HEAD_DIM), lambda i: (0, 0, 0)),
                  pl.BlockSpec((BLOCK, 128), lambda i: (i, 0))],
        out_specs=[pl.BlockSpec((HEADS, STEPS, 1, ROWS, HEAD_DIM), lambda i: (0, 0, i, 0, 0)),
                   pl.BlockSpec((HEADS, BLOCK, HEAD_DIM), lambda i: (0, i, 0))],
        name="rotate_heads",
    )(qkv, ssq, gains, table)


def attend_scatter(q_ref, k_ref, qkv_ref, wo_ref, x_ref, out_ref,
                   q_v, k_v, v_v, wo_v, o_v, ysend, recv0, s1, r1, keep, fin, s2, r2, x_v, ost,
                   ld_sem, wo_sem, x_sem, out_sem, y_send, y_recv, s1_send, s1_recv, s2_send, s2_recv):
    place = Place()
    scale = float(HEAD_DIM ** -0.5 * np.log2(np.e))

    def loads(h):
        return (pltpu.make_async_copy(q_ref.at[h], q_v.at[h], ld_sem.at[0, h]),
                pltpu.make_async_copy(k_ref.at[h], k_v.at[h], ld_sem.at[1, h]),
                pltpu.make_async_copy(qkv_ref.at[2, h], v_v.at[h], ld_sem.at[2, h]))

    for h in range(HEADS):
        for c in loads(h):
            c.start()
    pltpu.make_async_copy(wo_ref, wo_v, wo_sem).start()
    barrier_with(place, (SIB, XN, YN))

    def remote(src, dst, send, recv, kind):
        return pltpu.make_async_remote_copy(src_ref=src, dst_ref=dst, send_sem=send, recv_sem=recv,
                                            device_id=place.dev(place.kind(kind)), device_id_type=MESH)

    def to_sib(s):
        return remote(ysend, recv0.at[s % 2], y_send, y_recv.at[s % 2], SIB)

    def hop1(s, half):
        b = s % 2
        return remote(s1.at[b, half], r1.at[b, half], s1_send.at[b, half], s1_recv.at[b, half], (XN, YN)[half])

    def hop2(s, half):
        b = s % 2
        return remote(s2.at[b, half], r2.at[b, half], s2_send.at[b, half], s2_recv.at[b, half], (YN, XN)[half])

    def x_load(s):
        return pltpu.make_async_copy(x_ref.at[pl.ds(pl.multiple_of(s * ROWS, ROWS), ROWS)], x_v, x_sem)

    def out_store(s):
        return pltpu.make_async_copy(ost.at[s % 2], out_ref.at[pl.ds(pl.multiple_of(s * ROWS, ROWS), ROWS)], out_sem.at[s % 2])

    def gathered(b, half, other_core):
        c = place.core + other_core * (1 - 2 * place.core)
        order = ((0, 0), (0, 1), (1, 0), (1, 1)) if half == 0 else ((0, 0), (1, 0), (0, 1), (1, 1))
        parts = []
        for fx, fy in order:
            d = place.at(fx, fy, 0) // 2 * 2 + c
            parts.append(o_v[b, pl.ds(pl.multiple_of(d * ROWS, ROWS), ROWS), :])
        return jnp.concatenate(parts, axis=0)

    def tiles(body):
        def run(t, c):
            body(pl.ds(pl.multiple_of(t * TILE, TILE), TILE), t)
            return c
        lax.fori_loop(0, HALF // TILE, run, 0)

    def wo_tile(half, t):
        return wo_v[:, pl.ds(pl.multiple_of(half * HALF + t * TILE, TILE), TILE)]

    def project_sib(s):
        b = s % 2

        @pl.when(s >= 1)
        def _():
            to_sib(s - 1).wait_send()

        for half in range(2):
            rows = gathered(b, half, 1)

            def body(cols, t, half=half, rows=rows):
                ysend[half, :, cols] = jnp.dot(rows, wo_tile(half, t), preferred_element_type=F32).astype(BF16)
            tiles(body)
        to_sib(s).start()

    def stage1(s):
        b = s % 2
        to_sib(s).wait_recv()

        @pl.when(s >= 2)
        def _():
            for half in range(2):
                hop1(s - 2, half).wait_send()

        for half in range(2):
            rows = gathered(b, half, 0)

            def body(cols, t, half=half, rows=rows):
                y = jnp.dot(rows, wo_tile(half, t), preferred_element_type=F32) + recv0[b, half, :, cols].astype(F32)
                keep[half, :, cols] = y[:128]
                s1[b, half, :, cols] = y[128:].astype(BF16)
            tiles(body)
            hop1(s, half).start()

    def stage2(s):
        b = s % 2

        @pl.when(s >= 2)
        def _():
            for half in range(2):
                hop2(s - 2, half).wait_send()

        for half in range(2):
            hop1(s, half).wait_recv()

            def body(cols, t, half=half):
                y = keep[half, :, cols] + r1[b, half, :, cols].astype(F32)
                fin[half, :, cols] = y[:ROWS]
                s2[b, half, :, cols] = y[ROWS:].astype(BF16)
            tiles(body)
            hop2(s, half).start()

    def stage3(s):
        b = s % 2
        x_load(s).wait()

        @pl.when(s >= 2)
        def _():
            out_store(s - 2).wait()

        for half in range(2):
            hop2(s, half).wait_recv()

            def body(cols, t, half=half):
                y = (fin[half, :, cols] + r2[b, half, :, cols].astype(F32)).astype(BF16).astype(F32)
                whole = pl.ds(pl.multiple_of(half * HALF + t * TILE, TILE), TILE)
                ost[b, :, whole] = (x_v[:, whole].astype(F32) + y).astype(BF16)
            tiles(body)
        out_store(s).start()

    def attend(i, h):
        q = q_v[h, i]
        dims = (((1,), (1,)), ((), ()))

        def scores(j):
            return lax.dot_general(q[j * ROWS:], k_v[h, j * BLOCK:(j + 1) * BLOCK, :], dims, preferred_element_type=F32)

        row = lax.broadcasted_iota(jnp.int32, (ROWS, BLOCK), 0) + i * ROWS
        keep_mask = lax.broadcasted_iota(jnp.int32, (ROWS, BLOCK), 1) <= row
        m = l = acc = None
        ahead = scores(0)
        for j in range(TP):
            s = ahead
            if j + 1 < TP:
                ahead = scores(j + 1)
            top = jnp.where(keep_mask, s[:ROWS], -1e30)
            s = top if j == TP - 1 else jnp.concatenate([top, s[ROWS:]], axis=0)
            peak = jnp.max(s, axis=1, keepdims=True) * scale
            new_m = peak if j == 0 else jnp.maximum(m, peak)
            p = jnp.exp2(s * scale - new_m)
            part = p[:, 0:128]
            for c in range(1, BLOCK // 128):
                part = part + p[:, c * 128:(c + 1) * 128]
            pv = jnp.dot(p.astype(BF16), v_v[h, j * BLOCK:(j + 1) * BLOCK, :], preferred_element_type=F32)
            if j == 0:
                l, acc = part, pv
            else:
                alpha = jnp.exp2(m - new_m)
                l = l * alpha + part
                acc = acc * alpha + pv
            total = jnp.sum(l[:ROWS], axis=1, keepdims=True)
            o_v[i % 2, j * ROWS:(j + 1) * ROWS, pl.ds(pl.multiple_of(h * HEAD_DIM, HEAD_DIM), HEAD_DIM)] = (
                acc[:ROWS] / total).astype(BF16)
            if j + 1 < TP:
                m, l, acc = new_m[ROWS:], l[ROWS:], acc[ROWS:]

    def step(i, carry):
        @pl.when(i >= 3)
        def _():
            x_load(i - 3).start()

        def head(h, c):
            @pl.when(h == 1)
            def _():
                @pl.when(i >= 3)
                def _():
                    stage3(i - 3)

                @pl.when((i >= 2) & (i < STEPS + 2))
                def _():
                    stage2(i - 2)

                @pl.when((i >= 1) & (i < STEPS + 1))
                def _():
                    stage1(i - 1)

            @pl.when(i < STEPS)
            def _():
                @pl.when(i == 0)
                def _():
                    for cp in loads(h):
                        cp.wait()
                attend(i, h)
            return c

        lax.fori_loop(0, HEADS, head, 0)

        @pl.when(i < STEPS)
        def _():
            @pl.when(i == 0)
            def _():
                pltpu.make_async_copy(wo_ref, wo_v, wo_sem).wait()
            project_sib(i)
        return carry

    lax.fori_loop(0, STEPS + 3, step, 0)
    to_sib(STEPS - 1).wait_send()
    for s in (STEPS - 2, STEPS - 1):
        for half in range(2):
            hop1(s, half).wait_send()
            hop2(s, half).wait_send()
        out_store(s).wait()


def attend_scatter_call(q, k, qkv, wo, x):
    any_spec = pl.BlockSpec(memory_space=pl.ANY)
    return pl.pallas_call(
        attend_scatter,
        out_shape=jax.ShapeDtypeStruct((BLOCK, WIDTH), BF16),
        in_specs=[any_spec] * 5,
        out_specs=any_spec,
        scratch_shapes=[
            pltpu.VMEM((HEADS, STEPS, BLOCK, HEAD_DIM), BF16),
            pltpu.VMEM((HEADS, SEQ, HEAD_DIM), BF16),
            pltpu.VMEM((HEADS, SEQ, HEAD_DIM), BF16),
            pltpu.VMEM((COLS, WIDTH), BF16),
            pltpu.VMEM((2, BLOCK, COLS), BF16),
            pltpu.VMEM((2, 4 * ROWS, HALF), BF16),
            pltpu.VMEM((2, 2, 4 * ROWS, HALF), BF16),
            pltpu.VMEM((2, 2, 2 * ROWS, HALF), BF16),
            pltpu.VMEM((2, 2, 2 * ROWS, HALF), BF16),
            pltpu.VMEM((2, 2 * ROWS, HALF), F32),
            pltpu.VMEM((2, ROWS, HALF), F32),
            pltpu.VMEM((2, 2, ROWS, HALF), BF16),
            pltpu.VMEM((2, 2, ROWS, HALF), BF16),
            pltpu.VMEM((ROWS, WIDTH), BF16),
            pltpu.VMEM((2, ROWS, WIDTH), BF16),
            pltpu.SemaphoreType.DMA((3, HEADS)),
            pltpu.SemaphoreType.DMA(()),
            pltpu.SemaphoreType.DMA(()),
            pltpu.SemaphoreType.DMA((2,)),
            pltpu.SemaphoreType.DMA(()),
            pltpu.SemaphoreType.DMA((2,)),
            pltpu.SemaphoreType.DMA((2, 2)),
            pltpu.SemaphoreType.DMA((2, 2)),
            pltpu.SemaphoreType.DMA((2, 2)),
            pltpu.SemaphoreType.DMA((2, 2)),
        ],
        compiler_params=pltpu.CompilerParams(collective_id=1, has_side_effects=True, vmem_limit_bytes=62 * 2**20),
        name="attend_scatter",
    )(q, k, qkv, wo, x)


def rope_table():
    half = HEAD_DIM // 2
    freq = (10000.0 ** (-np.arange(half, dtype=np.float64) * (2.0 / HEAD_DIM))).astype(np.float32)
    angle = (np.arange(SEQ, dtype=np.float32)[:, None] * freq[None, :]).astype(np.float64)
    return np.concatenate([np.cos(angle), np.sin(angle)], axis=1).astype(np.float32)


def solution(mesh):
    table = rope_table()

    def local_block(x_local, attn_gain, wq, wk, wv, q_gain, k_gain, wo):
        x = x_local[0]
        xf = x.astype(F32)
        inv = lax.rsqrt(jnp.mean(xf * xf, axis=-1, keepdims=True) + 1e-5)
        h = (xf * inv * attn_gain).astype(BF16)
        qkv, ssq, _ = gather_project_call(h, wq, wk, wv)
        gains = jnp.stack([q_gain, k_gain]).reshape(2, HEADS, HEAD_DIM)
        q, k = rotate_heads_call(qkv, ssq, gains, jnp.asarray(table))
        q = q.reshape(HEADS, STEPS, BLOCK, HEAD_DIM)
        out = attend_scatter_call(q, k, qkv, wo, x)
        k_cache = jnp.transpose(k, (1, 0, 2))[None]
        v_cache = jnp.transpose(qkv[2], (1, 0, 2))[None]
        return out[None], k_cache, v_cache

    seq_spec = P("dp", "tp", None)
    head_spec = P("dp", None, "tp", None)
    col_spec = P(None, "tp")
    return jax.shard_map(local_block, mesh=mesh,
                         in_specs=(seq_spec, P(None), col_spec, col_spec, col_spec, P("tp"), P("tp"), P("tp", None)),
                         out_specs=(seq_spec, head_spec, head_spec), check_vma=False)
```

```python
import functools

import jax
import jax.numpy as jnp
import numpy as np
from jax import lax
from jax.experimental import pallas as pl
from jax.experimental.pallas import tpu as pltpu
from jax.sharding import PartitionSpec as P

MESH = pl.DeviceIdType.MESH
HEAD_DIM = 128
HEADS = 5
COLS = HEADS * HEAD_DIM
WIDTH = 5120
BLOCK = 512
TP = 8
SEQ = TP * BLOCK
PIECES = 4
PIECE = BLOCK // PIECES
UNIT = 256
STEPS = 8
ROWS = BLOCK // STEPS
HALF = WIDTH // 2
TILE = 512
LAG = 4
WO_PARTS = 8
WO_ROWS = COLS // WO_PARTS
F32 = jnp.float32
BF16 = jnp.bfloat16
SIB, XN, YN, DG, SX, SY, SDG = range(7)


class Place:
    def __init__(self):
        me = lax.axis_index("tp")
        self.dp = lax.axis_index("dp")
        self.me = me
        self.core = me % 2
        self.x = (me // 2) % 2
        self.y = me // 4

    def at(self, fx, fy, fc):
        x = self.x + fx * (1 - 2 * self.x)
        y = self.y + fy * (1 - 2 * self.y)
        c = self.core + fc * (1 - 2 * self.core)
        return (y * 2 + x) * 2 + c

    def kind(self, k):
        fx, fy, fc = ((0, 0, 1), (1, 0, 0), (0, 1, 0), (1, 1, 0), (1, 0, 1), (0, 1, 1), (1, 1, 1))[k]
        return self.at(fx, fy, fc)

    def dev(self, index):
        return (self.dp, index)


def barrier_with(place, kinds):
    sem = pltpu.get_barrier_semaphore()
    for k in kinds:
        pl.semaphore_signal(sem, inc=1, device_id=place.dev(place.kind(k)), device_id_type=MESH)
    pl.semaphore_wait(sem, len(kinds))


def diagonal():
    r = lax.broadcasted_iota(jnp.int32, (128, 128), 0)
    c = lax.broadcasted_iota(jnp.int32, (128, 128), 1)
    return r == c


def block_kernel(h_ref, wq_ref, wk_ref, wv_ref, wo_ref, x_ref, gain_ref, tab_ref, out_ref, k_ref, v_ref, hbuf,
                 qkv, ssq_v, ssq_all, wr, o_in, recv0, r1,
                 w_sem, h_sem, send_sem, recv_sem, ss_send, ss_recv, ss_loc, kv_sem,
                 wo_send, wo_recv, wo_sem, tab_sem, o_send, o_recv, x_sem, out_sem, y_send, y_recv, s1_send, s1_recv):
    place = Place()
    scale = float(HEAD_DIM ** -0.5 * np.log2(np.e))
    eye = diagonal()
    weights = (wq_ref, wk_ref, wv_ref)

    def remote(src, dst, send, recv, kind):
        return pltpu.make_async_remote_copy(src_ref=src, dst_ref=dst, send_sem=send, recv_sem=recv,
                                            device_id=place.dev(place.kind(kind)), device_id_type=MESH)

    def copy(src_ref, block, p, send, kind, target):
        return remote(src_ref, hbuf.at[block, pl.ds(p * PIECE, PIECE)], send_sem.at[send, p], recv_sem.at[kind, p], target)

    def own(p, send, kind):
        return copy(h_ref.at[pl.ds(p * PIECE, PIECE)], place.me, p, send, kind, kind)

    def relay(owner, p, send, kind, target):
        block = place.kind(owner)
        return copy(hbuf.at[block, pl.ds(p * PIECE, PIECE)], block, p, send, kind, target)

    def arrived(kind, p):
        relay(kind, p, 0, kind, SIB).wait_recv()

    def forwards(p):
        out = [(XN, p, 3, SX, SIB), (YN, p, 4, SY, SIB)]
        out.append((XN, p, 5, DG, YN) if p % 2 == 0 else (YN, p, 5, DG, XN))
        return out

    def wo_part(c, half):
        rows = pl.ds(c * WO_ROWS, WO_ROWS)
        return remote(wo_ref.at[rows, pl.ds(half * HALF, HALF)], wr.at[half, rows],
                      wo_send.at[half, c], wo_recv.at[half, c], (XN, YN)[half])

    def share(k):
        return remote(ssq_v, ssq_all.at[place.me], ss_send.at[k], ss_recv.at[k], k)

    def shared(k):
        return remote(ssq_v, ssq_all.at[place.kind(k)], ss_send.at[k], ss_recv.at[k], k)

    def v_store():
        return pltpu.make_async_copy(qkv.at[2], v_ref, kv_sem.at[1])

    def k_store():
        return pltpu.make_async_copy(qkv.at[1], k_ref, kv_sem.at[0])

    def unit(u):
        a = u // 4
        v = u - 4
        w = v % 4
        z = u - 12
        near = a == 0
        far = a == 3
        fc = jnp.where(near, u // 2, jnp.where(far, z % 2, w // 2))
        half = jnp.where(near, u % 2, jnp.where(far, z // 2, v // 4))
        fy = jnp.where(near, 0, jnp.where(far, 1, w % 2))
        fx = jnp.where(near, 0, jnp.where(far, 1, 1 - w % 2))
        return place.at(fx, fy, fc), half

    def project_phase(w_v, h_v):
        for n, w in enumerate(weights):
            pltpu.make_async_copy(w, w_v.at[n], w_sem.at[n]).start()
        barrier_with(place, range(7))
        for p in range(PIECES):
            own(p, 0, XN).start()
            own(p, 1, YN).start()
            own(p, 2, SIB).start()

        def load(u, slot, own_rows):
            block, half = unit(u)
            rows = pl.ds(pl.multiple_of(half * UNIT, UNIT), UNIT)
            if own_rows:
                return pltpu.make_async_copy(h_ref.at[rows], h_v.at[slot], h_sem.at[slot])
            return pltpu.make_async_copy(hbuf.at[block, rows], h_v.at[slot], h_sem.at[slot])

        def start_load(u):
            @pl.when(u < 2)
            def _():
                load(u, u % 2, True).start()

            @pl.when(u >= 2)
            def _():
                load(u, u % 2, False).start()

        def step(u, carry):
            slot = u % 2
            for first, p0 in ((4, 0), (8, 2)):
                @pl.when(u == first)
                def _(p0=p0):
                    for p in (p0, p0 + 1):
                        arrived(XN, p)
                        arrived(YN, p)
                        for f in forwards(p):
                            relay(*f).start()
            for first, p0 in ((12, 0), (14, 2)):
                @pl.when(u == first)
                def _(p0=p0, first=first):
                    for p in (p0, p0 + 1):
                        arrived(DG, p)
                        relay(DG, p, 6, SDG, SIB).start()
                    if first == 14:
                        for half in range(2):
                            wo_part(0, half).start()

            @pl.when((u % 4 == 0) | (u == 14))
            def _():
                start_load(u)

            for nxt, kind, p0 in ((2, SIB, 0), (3, SIB, 2), (6, SX, 0), (7, SY, 0), (10, SX, 2), (11, SY, 2), (13, SDG, 0), (15, SDG, 2)):
                @pl.when(u + 1 == nxt)
                def _(kind=kind, p0=p0):
                    arrived(kind, p0)
                    arrived(kind, p0 + 1)

            @pl.when(((u + 1) % 4 != 0) & (u + 1 != 14))
            def _():
                start_load(u + 1)

            @pl.when(u == 0)
            def _():
                for n, w in enumerate(weights):
                    pltpu.make_async_copy(w, w_v.at[n], w_sem.at[n]).wait()

            load(u, slot, False).wait()
            block, half = unit(u)
            rows = pl.ds(pl.multiple_of(block * BLOCK + half * UNIT, UNIT), UNIT)

            def part(n, c):
                r = jnp.dot(h_v[slot], w_v[n], preferred_element_type=F32).astype(BF16)
                for h in range(HEADS):
                    qkv[n, h, rows, :] = r[:, h * HEAD_DIM:(h + 1) * HEAD_DIM]

                @pl.when(n < 2)
                def _():
                    rf = r.astype(F32)
                    col = jnp.sum(rf * rf, axis=1, keepdims=True)
                    for b in range(UNIT // 128):
                        row = jnp.sum(jnp.where(eye, col[b * 128:(b + 1) * 128], 0.0), axis=0, keepdims=True)
                        ssq_v[pl.ds(block * 8 + n * 4 + half * 2 + b, 1), :] = row
                return c

            lax.fori_loop(0, 3, part, 0)
            return carry

        lax.fori_loop(0, 16, step, 0)

    pl.run_scoped(project_phase, pltpu.VMEM((3, WIDTH, COLS), BF16), pltpu.VMEM((2, UNIT, WIDTH), BF16))

    for k in range(7):
        share(k).start()
    mine = pltpu.make_async_copy(ssq_v, ssq_all.at[place.me], ss_loc)
    mine.start()
    for c in range(1, WO_PARTS):
        for half in range(2):
            wo_part(c, half).start()
    v_store().start()

    def to_sib(ysend, s):
        return remote(ysend, recv0.at[s % 2], y_send, y_recv.at[s % 2], SIB)

    def hop(s1, s, half):
        b = s % 2
        return remote(s1.at[b, half], r1.at[b, half], s1_send.at[b, half], s1_recv.at[b, half], (YN, XN)[half])

    def o_part(o_v, s, half, n):
        chip = place.at(*((1, 0, 0), (0, 1, 0))[half]) // 2 if n == 0 else place.at(1, 1, 0) // 2
        rows = pl.ds(pl.multiple_of(chip * 2 * ROWS, 2 * ROWS), 2 * ROWS)
        return remote(o_v.at[s, rows], o_in.at[half, s, n], o_send.at[half, s, n], o_recv.at[half, s, n], (XN, YN)[half])

    def attend_phase(wo_v, o_v, tab_v, ysend, yown, s1, keep, x_v, ost):
        tab = pltpu.make_async_copy(tab_ref, tab_v, tab_sem)
        tab.start()

        def wo_load(half):
            return pltpu.make_async_copy(wo_ref.at[:, pl.ds(half * HALF, HALF)], wo_v.at[half], wo_sem.at[half])

        for half in range(2):
            wo_load(half).start()
        mine.wait()
        for k in range(7):
            shared(k).wait_recv()
        tab.wait()
        low = lax.broadcasted_iota(jnp.int32, (128, 128), 1) < 64

        def rotate(g, carry):
            rows = pl.ds(pl.multiple_of(g * 128, 128), 128)
            t = tab_v[rows, :]
            turned = pltpu.roll(t, 64, 1)
            cos = jnp.where(low, t, turned)
            sin = jnp.where(low, -turned, t)
            for n in range(2):
                at = g // 4 * 8 + n * 4 + g % 4
                total = jnp.sum(ssq_all[:, pl.ds(at, 1), :], axis=0)
                col = jnp.sum(jnp.where(eye, total, 0.0), axis=1, keepdims=True)
                inv = lax.rsqrt(col / WIDTH + 1e-5)
                for h in range(HEADS):
                    x = qkv[n, h, rows, :].astype(F32) * inv * gain_ref[n, h:h + 1, :]
                    qkv[n, h, rows, :] = (x * cos + pltpu.roll(x, 64, 1) * sin).astype(BF16)
            return carry

        lax.fori_loop(0, SEQ // 128, rotate, 0)
        k_store().start()

        def x_load(s):
            return pltpu.make_async_copy(x_ref.at[pl.ds(pl.multiple_of(s * ROWS, ROWS), ROWS)], x_v, x_sem)

        def out_store(s):
            return pltpu.make_async_copy(ost.at[s % 2], out_ref.at[pl.ds(pl.multiple_of(s * ROWS, ROWS), ROWS)], out_sem.at[s % 2])

        def tiles(body):
            def run(t, c):
                body(pl.ds(pl.multiple_of(t * TILE, TILE), TILE), t)
                return c
            lax.fori_loop(0, HALF // TILE, run, 0)

        def operand(s, half):
            rows = []
            for fc in (1, 0):
                for n, far in enumerate(((0, 0), ((0, 1), (1, 0))[half])):
                    d = place.at(far[0], far[1], fc)
                    mine_o = o_v[s, pl.ds(pl.multiple_of(d * ROWS, ROWS), ROWS), :]
                    theirs = o_in[half, s, n, pl.ds(pl.multiple_of(d % 2 * ROWS, ROWS), ROWS), :]
                    rows.append(jnp.concatenate([mine_o, theirs], axis=1))
            return jnp.concatenate(rows, axis=0)

        def stage_b(s):
            @pl.when(s == 0)
            def _():
                for half in range(2):
                    wo_load(half).wait()
                    for c in range(WO_PARTS):
                        wo_part(c, half).wait_recv()

            @pl.when(s >= 1)
            def _():
                to_sib(ysend, s - 1).wait_send()

            for half in range(2):
                for n in range(2):
                    o_part(o_v, s, half, n).wait_recv()
                rows = operand(s, half)

                def body(cols, t, half=half, rows=rows):
                    w = jnp.concatenate([wo_v[half, :, cols], wr[half, :, cols]], axis=0)
                    y = jnp.dot(rows, w, preferred_element_type=F32)
                    ysend[half, :, cols] = y[:2 * ROWS].astype(BF16)
                    yown[half, :, cols] = y[2 * ROWS:]
                tiles(body)
            to_sib(ysend, s).start()

        def stage_c(s):
            b = s % 2
            to_sib(ysend, s).wait_recv()

            @pl.when(s >= 2)
            def _():
                for half in range(2):
                    hop(s1, s - 2, half).wait_send()

            for half in range(2):
                def body(cols, t, half=half):
                    y = yown[half, :, cols] + recv0[b, half, :, cols].astype(F32)
                    keep[half, :, cols] = y[:ROWS]
                    s1[b, half, :, cols] = y[ROWS:].astype(BF16)
                tiles(body)
                hop(s1, s, half).start()

        def stage_d(s):
            b = s % 2
            x_load(s).wait()

            @pl.when(s >= 2)
            def _():
                out_store(s - 2).wait()

            for half in range(2):
                hop(s1, s, half).wait_recv()

                def body(cols, t, half=half):
                    y = (keep[half, :, cols] + r1[b, half, :, cols].astype(F32)).astype(BF16).astype(F32)
                    whole = pl.ds(pl.multiple_of(half * HALF + t * TILE, TILE), TILE)
                    ost[b, :, whole] = (x_v[:, whole].astype(F32) + y).astype(BF16)
                tiles(body)
            out_store(s).start()

        def attend(i, h):
            q = jnp.concatenate([qkv[0, h, pl.ds(pl.multiple_of(d * BLOCK + i * ROWS, ROWS), ROWS), :] for d in range(TP)], axis=0)
            dims = (((1,), (1,)), ((), ()))

            def scores(j):
                return lax.dot_general(q[j * ROWS:], qkv[1, h, j * BLOCK:(j + 1) * BLOCK, :], dims, preferred_element_type=F32)

            row = lax.broadcasted_iota(jnp.int32, (ROWS, BLOCK), 0) + i * ROWS
            keep_mask = lax.broadcasted_iota(jnp.int32, (ROWS, BLOCK), 1) <= row
            m = l = acc = None
            ahead = scores(0)
            for j in range(TP):
                s = ahead
                if j + 1 < TP:
                    ahead = scores(j + 1)
                top = jnp.where(keep_mask, s[:ROWS], -1e30)
                s = top if j == TP - 1 else jnp.concatenate([top, s[ROWS:]], axis=0)
                peak = jnp.max(s, axis=1, keepdims=True) * scale
                new_m = peak if j == 0 else jnp.maximum(m, peak)
                p = jnp.exp2(s * scale - new_m)
                part = p[:, 0:128]
                for c in range(1, BLOCK // 128):
                    part = part + p[:, c * 128:(c + 1) * 128]
                pv = jnp.dot(p.astype(BF16), qkv[2, h, j * BLOCK:(j + 1) * BLOCK, :], preferred_element_type=F32)
                if j == 0:
                    l, acc = part, pv
                else:
                    alpha = jnp.exp2(m - new_m)
                    l = l * alpha + part
                    acc = acc * alpha + pv
                total = jnp.sum(l[:ROWS], axis=1, keepdims=True)
                o_v[i, j * ROWS:(j + 1) * ROWS, pl.ds(pl.multiple_of(h * HEAD_DIM, HEAD_DIM), HEAD_DIM)] = (
                    acc[:ROWS] / total).astype(BF16)
                if j + 1 < TP:
                    m, l, acc = new_m[ROWS:], l[ROWS:], acc[ROWS:]

        def step(i, carry):
            d = i - LAG - 2
            c = i - LAG - 1

            @pl.when(d >= 0)
            def _():
                x_load(d).start()

            def head(h, z):
                @pl.when(h == 1)
                def _():
                    @pl.when(d >= 0)
                    def _():
                        stage_d(d)

                    @pl.when((c >= 0) & (c < STEPS))
                    def _():
                        stage_c(c)

                @pl.when(i < STEPS)
                def _():
                    attend(i, h)
                return z

            lax.fori_loop(0, HEADS, head, 0)

            @pl.when(i < STEPS)
            def _():
                for half in range(2):
                    for n in range(2):
                        o_part(o_v, i, half, n).start()

            @pl.when((i >= LAG) & (i < STEPS + LAG))
            def _():
                stage_b(i - LAG)
            return carry

        lax.fori_loop(0, STEPS + LAG + 2, step, 0)
        to_sib(ysend, STEPS - 1).wait_send()
        for s in (STEPS - 2, STEPS - 1):
            for half in range(2):
                hop(s1, s, half).wait_send()
            out_store(s).wait()
        for s in range(STEPS):
            for half in range(2):
                for n in range(2):
                    o_part(o_v, s, half, n).wait_send()

    pl.run_scoped(attend_phase,
                  pltpu.VMEM((2, COLS, HALF), BF16),
                  pltpu.VMEM((STEPS, BLOCK, COLS), BF16),
                  pltpu.VMEM((SEQ, 128), F32),
                  pltpu.VMEM((2, 2 * ROWS, HALF), BF16),
                  pltpu.VMEM((2, 2 * ROWS, HALF), F32),
                  pltpu.VMEM((2, 2, ROWS, HALF), BF16),
                  pltpu.VMEM((2, ROWS, HALF), F32),
                  pltpu.VMEM((ROWS, WIDTH), BF16),
                  pltpu.VMEM((2, ROWS, WIDTH), BF16))
    for p in range(PIECES):
        own(p, 0, XN).wait_send()
        own(p, 1, YN).wait_send()
        own(p, 2, SIB).wait_send()
        for f in forwards(p):
            relay(*f).wait_send()
        relay(DG, p, 6, SDG, SIB).wait_send()
    for k in range(7):
        share(k).wait_send()
    for half in range(2):
        for c in range(WO_PARTS):
            wo_part(c, half).wait_send()
    v_store().wait()
    k_store().wait()


def block_call(h, wq, wk, wv, wo, x, gains, table):
    any_spec = pl.BlockSpec(memory_space=pl.ANY)
    dma = pltpu.SemaphoreType.DMA
    return pl.pallas_call(
        block_kernel,
        out_shape=[jax.ShapeDtypeStruct((BLOCK, WIDTH), BF16),
                   jax.ShapeDtypeStruct((HEADS, SEQ, HEAD_DIM), BF16),
                   jax.ShapeDtypeStruct((HEADS, SEQ, HEAD_DIM), BF16),
                   jax.ShapeDtypeStruct((TP, BLOCK, WIDTH), BF16)],
        in_specs=[any_spec] * 6 + [pl.BlockSpec(memory_space=pltpu.VMEM), any_spec],
        out_specs=[any_spec] * 4,
        scratch_shapes=[
            pltpu.VMEM((3, HEADS, SEQ, HEAD_DIM), BF16),
            pltpu.VMEM((64, 128), F32),
            pltpu.VMEM((TP, 64, 128), F32),
            pltpu.VMEM((2, COLS, HALF), BF16),
            pltpu.VMEM((2, STEPS, 2, 2 * ROWS, COLS), BF16),
            pltpu.VMEM((2, 2, 2 * ROWS, HALF), BF16),
            pltpu.VMEM((2, 2, ROWS, HALF), BF16),
            dma((3,)), dma((2,)), dma((7, PIECES)), dma((7, PIECES)), dma((7,)), dma((7,)), dma(()), dma((2,)),
            dma((2, WO_PARTS)), dma((2, WO_PARTS)), dma((2,)), dma(()),
            dma((2, STEPS, 2)), dma((2, STEPS, 2)), dma(()), dma((2,)),
            dma(()), dma((2,)), dma((2, 2)), dma((2, 2)),
        ],
        compiler_params=pltpu.CompilerParams(collective_id=0, has_side_effects=True, vmem_limit_bytes=67043328),
        name="block",
    )(h, wq, wk, wv, wo, x, gains, table)


def rope_table():
    half = HEAD_DIM // 2
    freq = (10000.0 ** (-np.arange(half, dtype=np.float64) * (2.0 / HEAD_DIM))).astype(np.float32)
    angle = (np.arange(SEQ, dtype=np.float32)[:, None] * freq[None, :]).astype(np.float64)
    return np.concatenate([np.cos(angle), np.sin(angle)], axis=1).astype(np.float32)


def solution(mesh):
    table = rope_table()

    def local_block(x_local, attn_gain, wq, wk, wv, q_gain, k_gain, wo):
        x = x_local[0]
        xf = x.astype(F32)
        inv = lax.rsqrt(jnp.mean(xf * xf, axis=-1, keepdims=True) + 1e-5)
        h = (xf * inv * attn_gain).astype(BF16)
        gains = jnp.stack([q_gain, k_gain]).reshape(2, HEADS, HEAD_DIM)
        out, k, v, _ = block_call(h, wq, wk, wv, wo, x, gains, jnp.asarray(table))
        k_cache = jnp.transpose(k, (1, 0, 2))[None]
        v_cache = jnp.transpose(v, (1, 0, 2))[None]
        return out[None], k_cache, v_cache

    seq_spec = P("dp", "tp", None)
    head_spec = P("dp", None, "tp", None)
    col_spec = P(None, "tp")
    return jax.shard_map(local_block, mesh=mesh,
                         in_specs=(seq_spec, P(None), col_spec, col_spec, col_spec, P("tp"), P("tp"), P("tp", None)),
                         out_specs=(seq_spec, head_spec, head_spec), check_vma=False)
```

```python
import functools

import jax
import jax.numpy as jnp
import numpy as np
from jax import lax
from jax.experimental import pallas as pl
from jax.experimental.pallas import tpu as pltpu
from jax.sharding import PartitionSpec as P

MESH = pl.DeviceIdType.MESH
HEAD_DIM = 128
HEADS = 5
COLS = HEADS * HEAD_DIM
WIDTH = 5120
BLOCK = 512
TP = 8
SEQ = TP * BLOCK
PIECES = 8
PIECE = BLOCK // PIECES
UNIT = 128
STEPS = 8
ROWS = BLOCK // STEPS
HALF = WIDTH // 2
TILE = 512
LAG = 4
EARLY = 2
WO_PARTS = 10
WO_ROWS = COLS // WO_PARTS
F32 = jnp.float32
BF16 = jnp.bfloat16
SIB, XN, YN, DG, SX, SY, SDG = range(7)


class Place:
    def __init__(self):
        me = lax.axis_index("tp")
        self.dp = lax.axis_index("dp")
        self.me = me
        self.core = me % 2
        self.x = (me // 2) % 2
        self.y = me // 4

    def at(self, fx, fy, fc):
        x = self.x + fx * (1 - 2 * self.x)
        y = self.y + fy * (1 - 2 * self.y)
        c = self.core + fc * (1 - 2 * self.core)
        return (y * 2 + x) * 2 + c

    def kind(self, k):
        fx, fy, fc = ((0, 0, 1), (1, 0, 0), (0, 1, 0), (1, 1, 0), (1, 0, 1), (0, 1, 1), (1, 1, 1))[k]
        return self.at(fx, fy, fc)

    def dev(self, index):
        return (self.dp, index)


def barrier_signal(place, kinds):
    for k in kinds:
        pl.semaphore_signal(pltpu.get_barrier_semaphore(), inc=1, device_id=place.dev(place.kind(k)), device_id_type=MESH)


def barrier_wait(count):
    pl.semaphore_wait(pltpu.get_barrier_semaphore(), count)


def diagonal():
    r = lax.broadcasted_iota(jnp.int32, (128, 128), 0)
    c = lax.broadcasted_iota(jnp.int32, (128, 128), 1)
    return r == c


def block_kernel(x_ref, an_ref, wq_ref, wk_ref, wv_ref, qg_ref, kg_ref, wo_ref, tab_ref, out_ref, k_ref, v_ref, hbuf,
                 qkv, ssq_v, ssq_all, wr, o_in, recv0, r1,
                 w_sem, h_sem, n_sem, send_sem, recv_sem, ss_send, ss_recv, ss_loc, kv_sem,
                 wo_send, wo_recv, wo_sem, tab_sem, o_send, o_recv, x_sem, out_sem, y_send, y_recv, s1_send, s1_recv):
    place = Place()
    scale = float(HEAD_DIM ** -0.5 * np.log2(np.e))
    eye = diagonal()
    weights = (wq_ref, wk_ref, wv_ref)

    def remote(src, dst, send, recv, kind):
        return pltpu.make_async_remote_copy(src_ref=src, dst_ref=dst, send_sem=send, recv_sem=recv,
                                            device_id=place.dev(place.kind(kind)), device_id_type=MESH)

    def copy(src_ref, block, p, send, kind, target):
        return remote(src_ref, hbuf.at[block, pl.ds(p * PIECE, PIECE)], send_sem.at[send, p], recv_sem.at[kind, p], target)

    def own(p, send, kind):
        return copy(hbuf.at[place.me, pl.ds(p * PIECE, PIECE)], place.me, p, send, kind, kind)

    def relay(owner, p, send, kind, target):
        block = place.kind(owner)
        return copy(hbuf.at[block, pl.ds(p * PIECE, PIECE)], block, p, send, kind, target)

    def arrived(kind, p):
        relay(kind, p, 0, kind, SIB).wait_recv()

    def forwards(p):
        out = [(XN, p, 3, SX, SIB), (YN, p, 4, SY, SIB)]
        out.append((XN, p, 5, DG, YN) if p % 2 == 0 else (YN, p, 5, DG, XN))
        return out

    def wo_part(c, half):
        rows = pl.ds(c * WO_ROWS, WO_ROWS)
        return remote(wo_ref.at[rows, pl.ds(half * HALF, HALF)], wr.at[half, rows],
                      wo_send.at[half, c], wo_recv.at[half, c], (XN, YN)[half])

    def share(k):
        return remote(ssq_v, ssq_all.at[place.me], ss_send.at[k], ss_recv.at[k], k)

    def shared(k):
        return remote(ssq_v, ssq_all.at[place.kind(k)], ss_send.at[k], ss_recv.at[k], k)

    def v_store():
        return pltpu.make_async_copy(qkv.at[2], v_ref, kv_sem.at[1])

    def k_store():
        return pltpu.make_async_copy(qkv.at[1], k_ref, kv_sem.at[0])

    def unit(u):
        v = u - 8
        w = v % 4
        z = u - 24
        near = u < 8
        far = u >= 24
        fc = jnp.where(near, u // 4, jnp.where(far, z % 2, w // 2))
        part = jnp.where(near, u % 4, jnp.where(far, z // 2, v // 4))
        fy = jnp.where(near, 0, jnp.where(far, 1, w % 2))
        fx = jnp.where(near, 0, jnp.where(far, 1, 1 - w % 2))
        return place.at(fx, fy, fc), part

    def project_phase(w_v, h_v):
        def x_piece(p):
            return pltpu.make_async_copy(x_ref.at[pl.ds(p * PIECE, PIECE)], h_v.at[1, pl.ds(p % 2 * PIECE, PIECE)], n_sem.at[0, p % 2])

        def h_piece(p):
            return pltpu.make_async_copy(h_v.at[0, pl.ds(p % 2 * PIECE, PIECE)], hbuf.at[place.me, pl.ds(p * PIECE, PIECE)], n_sem.at[1, p % 2])

        x_piece(0).start()
        x_piece(1).start()
        for n, w in enumerate(weights):
            pltpu.make_async_copy(w, w_v.at[n], w_sem.at[n]).start()
        barrier_signal(place, range(7))
        for p in range(PIECES):
            x_piece(p).wait()

            def normalize(r, c, p=p):
                rows = pl.ds(pl.multiple_of(p % 2 * PIECE + r * 16, 16), 16)
                xf = h_v[1, rows, :].astype(F32)
                inv = lax.rsqrt(jnp.mean(xf * xf, axis=-1, keepdims=True) + 1e-5)
                h_v[0, rows, :] = (xf * inv * an_ref[...]).astype(BF16)
                return c

            lax.fori_loop(0, PIECE // 16, normalize, 0)
            h_piece(p).start()
            if p + 2 < PIECES:
                x_piece(p + 2).start()
            h_piece(p).wait()
            if p == 0:
                barrier_wait(7)
            own(p, 0, XN).start()
            own(p, 1, YN).start()
            own(p, 2, SIB).start()

        def load(u, slot):
            block, half = unit(u)
            rows = pl.ds(pl.multiple_of(half * UNIT, UNIT), UNIT)
            return pltpu.make_async_copy(hbuf.at[block, rows], h_v.at[slot], h_sem.at[slot])

        def start_load(u):
            load(u, u % 2).start()

        def step(u, carry):
            slot = u % 2
            for g in range(4):
                @pl.when(u == 8 + 4 * g)
                def _(g=g):
                    for p in (2 * g, 2 * g + 1):
                        arrived(XN, p)
                        arrived(YN, p)
                        for f in forwards(p):
                            relay(*f).start()

                @pl.when(u == 24 + 2 * g)
                def _(g=g):
                    for p in (2 * g, 2 * g + 1):
                        arrived(DG, p)
                        relay(DG, p, 6, SDG, SIB).start()
                    if g == 2:
                        for c in range(EARLY):
                            for half in range(2):
                                wo_part(c, half).start()

            def opens(t):
                return (t == 0) | ((t >= 8) & (t < 24) & (t % 4 == 0)) | ((t >= 24) & (t % 2 == 0))

            @pl.when(opens(u))
            def _():
                start_load(u)

            for g in range(4):
                for nxt, kind in ((4 + g, SIB), (10 + 4 * g, SX), (11 + 4 * g, SY), (25 + 2 * g, SDG)):
                    @pl.when(u + 1 == nxt)
                    def _(kind=kind, g=g):
                        arrived(kind, 2 * g)
                        arrived(kind, 2 * g + 1)

            @pl.when((u + 1 < 32) & jnp.logical_not(opens(u + 1)))
            def _():
                start_load(u + 1)

            @pl.when(u == 0)
            def _():
                for n, w in enumerate(weights):
                    pltpu.make_async_copy(w, w_v.at[n], w_sem.at[n]).wait()

            load(u, slot).wait()
            block, half = unit(u)
            rows = pl.ds(pl.multiple_of(block * BLOCK + half * UNIT, UNIT), UNIT)

            def part(n, c):
                r = jnp.dot(h_v[slot], w_v[n], preferred_element_type=F32).astype(BF16)
                for h in range(HEADS):
                    qkv[n, h, rows, :] = r[:, h * HEAD_DIM:(h + 1) * HEAD_DIM]

                @pl.when(n < 2)
                def _():
                    rf = r.astype(F32)
                    col = jnp.sum(rf * rf, axis=1, keepdims=True)
                    for b in range(UNIT // 128):
                        row = jnp.sum(jnp.where(eye, col[b * 128:(b + 1) * 128], 0.0), axis=0, keepdims=True)
                        ssq_v[pl.ds(block * 8 + n * 4 + half, 1), :] = row
                return c

            lax.fori_loop(0, 3, part, 0)
            return carry

        lax.fori_loop(0, 32, step, 0)

    pl.run_scoped(project_phase, pltpu.VMEM((3, WIDTH, COLS), BF16), pltpu.VMEM((2, UNIT, WIDTH), BF16))

    for k in range(7):
        share(k).start()
    mine = pltpu.make_async_copy(ssq_v, ssq_all.at[place.me], ss_loc)
    mine.start()
    for c in range(EARLY, WO_PARTS):
        for half in range(2):
            wo_part(c, half).start()
    v_store().start()

    def to_sib(ysend, s):
        return remote(ysend, recv0.at[s % 2], y_send, y_recv.at[s % 2], SIB)

    def hop(s1, s, half):
        b = s % 2
        return remote(s1.at[b, half], r1.at[s % 4, half], s1_send.at[b, half], s1_recv.at[s % 4, half], (YN, XN)[half])

    def o_part(o_v, s, half, n):
        chip = place.at(*((1, 0, 0), (0, 1, 0))[half]) // 2 if n == 0 else place.at(1, 1, 0) // 2
        rows = pl.ds(pl.multiple_of(chip * 2 * ROWS, 2 * ROWS), 2 * ROWS)
        return remote(o_v.at[s, rows], o_in.at[half, s, n], o_send.at[half, s, n], o_recv.at[half, s, n], (XN, YN)[half])

    def attend_phase(wo_v, o_v, tab_v, ysend, yown, s1, keep, x_v, ost):
        tab = pltpu.make_async_copy(tab_ref, tab_v, tab_sem)
        tab.start()

        def wo_load(half):
            return pltpu.make_async_copy(wo_ref.at[:, pl.ds(half * HALF, HALF)], wo_v.at[half], wo_sem.at[half])

        for half in range(2):
            wo_load(half).start()
        mine.wait()
        for k in range(7):
            shared(k).wait_recv()
        tab.wait()
        low = lax.broadcasted_iota(jnp.int32, (128, 128), 1) < 64
        gains = [[g[h * HEAD_DIM:(h + 1) * HEAD_DIM][None] for h in range(HEADS)] for g in (qg_ref, kg_ref)]

        def rotate(g, carry):
            rows = pl.ds(pl.multiple_of(g * 128, 128), 128)
            t = tab_v[rows, :]
            turned = pltpu.roll(t, 64, 1)
            cos = jnp.where(low, t, turned)
            sin = jnp.where(low, -turned, t)
            for n in range(2):
                at = g // 4 * 8 + n * 4 + g % 4
                total = jnp.sum(ssq_all[:, pl.ds(at, 1), :], axis=0)
                col = jnp.sum(jnp.where(eye, total, 0.0), axis=1, keepdims=True)
                inv = lax.rsqrt(col / WIDTH + 1e-5)
                for h in range(HEADS):
                    x = qkv[n, h, rows, :].astype(F32) * inv * gains[n][h]
                    qkv[n, h, rows, :] = (x * cos + pltpu.roll(x, 64, 1) * sin).astype(BF16)
            return carry

        lax.fori_loop(0, SEQ // 128, rotate, 0, unroll=2)
        k_store().start()

        def x_load(s):
            return pltpu.make_async_copy(x_ref.at[pl.ds(pl.multiple_of(s * ROWS, ROWS), ROWS)], x_v, x_sem)

        def out_store(s):
            return pltpu.make_async_copy(ost.at[s % 2], out_ref.at[pl.ds(pl.multiple_of(s * ROWS, ROWS), ROWS)], out_sem.at[s % 2])

        def tiles(body):
            def run(t, c):
                body(pl.ds(pl.multiple_of(t * TILE, TILE), TILE), t)
                return c
            lax.fori_loop(0, HALF // TILE, run, 0)

        def operand(s, half):
            rows = []
            for fc in (1, 0):
                for n, far in enumerate(((0, 0), ((0, 1), (1, 0))[half])):
                    d = place.at(far[0], far[1], fc)
                    mine_o = o_v[s, pl.ds(pl.multiple_of(d * ROWS, ROWS), ROWS), :]
                    theirs = o_in[half, s, n, pl.ds(pl.multiple_of(d % 2 * ROWS, ROWS), ROWS), :]
                    rows.append(jnp.concatenate([mine_o, theirs], axis=1))
            return jnp.concatenate(rows, axis=0)

        def stage_b(s):
            @pl.when(s == 0)
            def _():
                for half in range(2):
                    wo_load(half).wait()
                    for c in range(WO_PARTS):
                        wo_part(c, half).wait_recv()

            @pl.when(s >= 1)
            def _():
                to_sib(ysend, s - 1).wait_send()

            for half in range(2):
                for n in range(2):
                    o_part(o_v, s, half, n).wait_recv()
                rows = operand(s, half)

                def body(cols, t, half=half, rows=rows):
                    w = jnp.concatenate([wo_v[half, :, cols], wr[half, :, cols]], axis=0)
                    y = jnp.dot(rows, w, preferred_element_type=F32)
                    ysend[half, :, cols] = y[:2 * ROWS].astype(BF16)
                    yown[half, :, cols] = y[2 * ROWS:]
                tiles(body)
            to_sib(ysend, s).start()

        def stage_c(s):
            b = s % 2
            to_sib(ysend, s).wait_recv()

            @pl.when(s >= 2)
            def _():
                for half in range(2):
                    hop(s1, s - 2, half).wait_send()

            for half in range(2):
                def body(cols, t, half=half):
                    y = yown[half, :, cols] + recv0[b, half, :, cols].astype(F32)
                    keep[b, half, :, cols] = y[:ROWS]
                    s1[b, half, :, cols] = y[ROWS:].astype(BF16)
                tiles(body)
                hop(s1, s, half).start()

        def stage_d(s):
            b = s % 2
            x_load(s).wait()

            @pl.when(s >= 2)
            def _():
                out_store(s - 2).wait()

            for half in range(2):
                hop(s1, s, half).wait_recv()

                def body(cols, t, half=half):
                    y = (keep[b, half, :, cols] + r1[s % 4, half, :, cols].astype(F32)).astype(BF16).astype(F32)
                    whole = pl.ds(pl.multiple_of(half * HALF + t * TILE, TILE), TILE)
                    ost[b, :, whole] = (x_v[:, whole].astype(F32) + y).astype(BF16)
                tiles(body)
            out_store(s).start()

        def attend(i, h):
            q = jnp.concatenate([qkv[0, h, pl.ds(pl.multiple_of(d * BLOCK + i * ROWS, ROWS), ROWS), :] for d in range(TP)], axis=0)
            dims = (((1,), (1,)), ((), ()))

            def scores(j):
                return lax.dot_general(q[j * ROWS:], qkv[1, h, j * BLOCK:(j + 1) * BLOCK, :], dims, preferred_element_type=F32)

            row = lax.broadcasted_iota(jnp.int32, (ROWS, BLOCK), 0) + i * ROWS
            keep_mask = lax.broadcasted_iota(jnp.int32, (ROWS, BLOCK), 1) <= row
            m = l = acc = None
            ahead = scores(0)
            for j in range(TP):
                s = ahead
                if j + 1 < TP:
                    ahead = scores(j + 1)
                top = jnp.where(keep_mask, s[:ROWS], -1e30)
                s = top if j == TP - 1 else jnp.concatenate([top, s[ROWS:]], axis=0)
                peak = jnp.max(s, axis=1, keepdims=True) * scale
                new_m = peak if j == 0 else jnp.maximum(m, peak)
                p = jnp.exp2(s * scale - new_m)
                part = p[:, 0:128]
                for c in range(1, BLOCK // 128):
                    part = part + p[:, c * 128:(c + 1) * 128]
                pv = jnp.dot(p.astype(BF16), qkv[2, h, j * BLOCK:(j + 1) * BLOCK, :], preferred_element_type=F32)
                if j == 0:
                    l, acc = part, pv
                else:
                    alpha = jnp.exp2(m - new_m)
                    l = l * alpha + part
                    acc = acc * alpha + pv
                total = jnp.sum(l[:ROWS], axis=1, keepdims=True)
                o_v[i, j * ROWS:(j + 1) * ROWS, pl.ds(pl.multiple_of(h * HEAD_DIM, HEAD_DIM), HEAD_DIM)] = (
                    acc[:ROWS] / total).astype(BF16)
                if j + 1 < TP:
                    m, l, acc = new_m[ROWS:], l[ROWS:], acc[ROWS:]

        def substep(s):
            @pl.when((s >= 3) & (s < STEPS + 3))
            def _():
                stage_d(s - 3)

            @pl.when((s >= 2) & (s < STEPS + 2))
            def _():
                x_load(s - 2).start()

            @pl.when((s >= 1) & (s <= STEPS))
            def _():
                stage_c(s - 1)

            @pl.when((s >= 0) & (s < STEPS))
            def _():
                stage_b(s)

        def step(i, carry):
            def head(h, z):
                @pl.when(i < STEPS)
                def _():
                    attend(i, h)

                    @pl.when(h == HEADS - 1)
                    def _():
                        for half in range(2):
                            for n in range(2):
                                o_part(o_v, i, half, n).start()

                @pl.when((i >= LAG) & ((h == 1) | (h == HEADS - 1)))
                def _():
                    substep(2 * (i - LAG) + h // (HEADS - 1) - 1)
                return z

            lax.fori_loop(0, HEADS, head, 0)
            return carry

        lax.fori_loop(0, LAG + STEPS // 2 + 2, step, 0)
        to_sib(ysend, STEPS - 1).wait_send()
        for s in (STEPS - 2, STEPS - 1):
            for half in range(2):
                hop(s1, s, half).wait_send()
            out_store(s).wait()
        for s in range(STEPS):
            for half in range(2):
                for n in range(2):
                    o_part(o_v, s, half, n).wait_send()

    pl.run_scoped(attend_phase,
                  pltpu.VMEM((2, COLS, HALF), BF16),
                  pltpu.VMEM((STEPS, BLOCK, COLS), BF16),
                  pltpu.VMEM((SEQ, 128), F32),
                  pltpu.VMEM((2, 2 * ROWS, HALF), BF16),
                  pltpu.VMEM((2, 2 * ROWS, HALF), F32),
                  pltpu.VMEM((2, 2, ROWS, HALF), BF16),
                  pltpu.VMEM((2, 2, ROWS, HALF), F32),
                  pltpu.VMEM((ROWS, WIDTH), BF16),
                  pltpu.VMEM((2, ROWS, WIDTH), BF16))
    for p in range(PIECES):
        own(p, 0, XN).wait_send()
        own(p, 1, YN).wait_send()
        own(p, 2, SIB).wait_send()
        for f in forwards(p):
            relay(*f).wait_send()
        relay(DG, p, 6, SDG, SIB).wait_send()
    for k in range(7):
        share(k).wait_send()
    for half in range(2):
        for c in range(WO_PARTS):
            wo_part(c, half).wait_send()
    v_store().wait()
    k_store().wait()


def block_call(x, an, wq, wk, wv, qg, kg, wo, table):
    any_spec = pl.BlockSpec(memory_space=pl.ANY)
    vmem_spec = pl.BlockSpec(memory_space=pltpu.VMEM)
    dma = pltpu.SemaphoreType.DMA
    return pl.pallas_call(
        block_kernel,
        out_shape=[jax.ShapeDtypeStruct((BLOCK, WIDTH), BF16),
                   jax.ShapeDtypeStruct((HEADS, SEQ, HEAD_DIM), BF16),
                   jax.ShapeDtypeStruct((HEADS, SEQ, HEAD_DIM), BF16),
                   jax.ShapeDtypeStruct((TP, BLOCK, WIDTH), BF16)],
        in_specs=[any_spec, vmem_spec, any_spec, any_spec, any_spec, vmem_spec, vmem_spec, any_spec, any_spec],
        out_specs=[any_spec] * 4,
        scratch_shapes=[
            pltpu.VMEM((3, HEADS, SEQ, HEAD_DIM), BF16),
            pltpu.VMEM((64, 128), F32),
            pltpu.VMEM((TP, 64, 128), F32),
            pltpu.VMEM((2, COLS, HALF), BF16),
            pltpu.VMEM((2, STEPS, 2, 2 * ROWS, COLS), BF16),
            pltpu.VMEM((2, 2, 2 * ROWS, HALF), BF16),
            pltpu.VMEM((4, 2, ROWS, HALF), BF16),
            dma((3,)), dma((2,)), dma((2, 2)), dma((7, PIECES)), dma((7, PIECES)), dma((7,)), dma((7,)), dma(()), dma((2,)),
            dma((2, WO_PARTS)), dma((2, WO_PARTS)), dma((2,)), dma(()),
            dma((2, STEPS, 2)), dma((2, STEPS, 2)), dma(()), dma((2,)),
            dma(()), dma((2,)), dma((2, 2)), dma((4, 2)),
        ],
        compiler_params=pltpu.CompilerParams(collective_id=0, has_side_effects=True, vmem_limit_bytes=67043328),
        name="block",
    )(x, an, wq, wk, wv, qg, kg, wo, table)


def rope_table():
    half = HEAD_DIM // 2
    freq = (10000.0 ** (-np.arange(half, dtype=np.float64) * (2.0 / HEAD_DIM))).astype(np.float32)
    angle = (np.arange(SEQ, dtype=np.float32)[:, None] * freq[None, :]).astype(np.float64)
    return np.concatenate([np.cos(angle), np.sin(angle)], axis=1).astype(np.float32)


def solution(mesh):
    table = rope_table()

    def local_block(x_local, attn_gain, wq, wk, wv, q_gain, k_gain, wo):
        out, k, v, _ = block_call(x_local[0], attn_gain[None], wq, wk, wv, q_gain, k_gain, wo, jnp.asarray(table))
        k_cache = jnp.transpose(k, (1, 0, 2))[None]
        v_cache = jnp.transpose(v, (1, 0, 2))[None]
        return out[None], k_cache, v_cache

    seq_spec = P("dp", "tp", None)
    head_spec = P("dp", None, "tp", None)
    col_spec = P(None, "tp")
    return jax.shard_map(local_block, mesh=mesh,
                         in_specs=(seq_spec, P(None), col_spec, col_spec, col_spec, P("tp"), P("tp"), P("tp", None)),
                         out_specs=(seq_spec, head_spec, head_spec), check_vma=False)
```

```python
import functools

import jax
import jax.numpy as jnp
import numpy as np
from jax import lax
from jax.experimental import pallas as pl
from jax.experimental.pallas import tpu as pltpu
from jax.sharding import PartitionSpec as P

MESH = pl.DeviceIdType.MESH
HEAD_DIM = 128
HEADS = 5
COLS = HEADS * HEAD_DIM
WIDTH = 5120
BLOCK = 512
TP = 8
SEQ = TP * BLOCK
PIECES = 8
PIECE = BLOCK // PIECES
UNIT = 128
STEPS = 8
ROWS = BLOCK // STEPS
HALF = WIDTH // 2
TILE = 512
LAG = 4
EARLY = 2
WO_PARTS = 10
WO_ROWS = COLS // WO_PARTS
F32 = jnp.float32
BF16 = jnp.bfloat16
SIB, XN, YN, DG, SX, SY, SDG = range(7)


class Place:
    def __init__(self):
        me = lax.axis_index("tp")
        self.dp = lax.axis_index("dp")
        self.me = me
        self.core = me % 2
        self.x = (me // 2) % 2
        self.y = me // 4

    def at(self, fx, fy, fc):
        x = self.x + fx * (1 - 2 * self.x)
        y = self.y + fy * (1 - 2 * self.y)
        c = self.core + fc * (1 - 2 * self.core)
        return (y * 2 + x) * 2 + c

    def kind(self, k):
        fx, fy, fc = ((0, 0, 1), (1, 0, 0), (0, 1, 0), (1, 1, 0), (1, 0, 1), (0, 1, 1), (1, 1, 1))[k]
        return self.at(fx, fy, fc)

    def dev(self, index):
        return (self.dp, index)


def barrier_signal(place, kinds):
    for k in kinds:
        pl.semaphore_signal(pltpu.get_barrier_semaphore(), inc=1, device_id=place.dev(place.kind(k)), device_id_type=MESH)


def barrier_wait(count):
    pl.semaphore_wait(pltpu.get_barrier_semaphore(), count)


def diagonal():
    r = lax.broadcasted_iota(jnp.int32, (128, 128), 0)
    c = lax.broadcasted_iota(jnp.int32, (128, 128), 1)
    return r == c


def block_kernel(x_ref, an_ref, wq_ref, wk_ref, wv_ref, qg_ref, kg_ref, wo_ref, tab_ref, out_ref, k_ref, v_ref, hbuf,
                 q_ref, ssq_v, ssq_all, wr, o_in, recv0, r1,
                 w_sem, h_sem, n_sem, send_sem, recv_sem, ss_send, ss_recv, ss_loc,
                 wo_send, wo_recv, wo_sem, tab_sem, o_send, o_recv, x_sem, y_send, y_recv, s1_send, s1_recv):
    place = Place()
    scale = float(HEAD_DIM ** -0.5 * np.log2(np.e))
    eye = diagonal()
    weights = (wq_ref, wk_ref, wv_ref)

    def remote(src, dst, send, recv, kind):
        return pltpu.make_async_remote_copy(src_ref=src, dst_ref=dst, send_sem=send, recv_sem=recv,
                                            device_id=place.dev(place.kind(kind)), device_id_type=MESH)

    def copy(src_ref, block, p, send, kind, target):
        return remote(src_ref, hbuf.at[block, pl.ds(p * PIECE, PIECE)], send_sem.at[send, p], recv_sem.at[kind, p], target)

    def own(p, send, kind):
        return copy(hbuf.at[place.me, pl.ds(p * PIECE, PIECE)], place.me, p, send, kind, kind)

    def relay(owner, p, send, kind, target):
        block = place.kind(owner)
        return copy(hbuf.at[block, pl.ds(p * PIECE, PIECE)], block, p, send, kind, target)

    def arrived(kind, p):
        relay(kind, p, 0, kind, SIB).wait_recv()

    def forwards(p):
        out = [(XN, p, 3, SX, SIB), (YN, p, 4, SY, SIB)]
        out.append((XN, p, 5, DG, YN) if p % 2 == 0 else (YN, p, 5, DG, XN))
        return out

    def wo_part(c, half):
        rows = pl.ds(c * WO_ROWS, WO_ROWS)
        return remote(wo_ref.at[rows, pl.ds(half * HALF, HALF)], wr.at[half, rows],
                      wo_send.at[half, c], wo_recv.at[half, c], (XN, YN)[half])

    def share(k):
        return remote(ssq_v, ssq_all.at[place.me], ss_send.at[k], ss_recv.at[k], k)

    def shared(k):
        return remote(ssq_v, ssq_all.at[place.kind(k)], ss_send.at[k], ss_recv.at[k], k)

    qkv = (q_ref, k_ref, v_ref)

    def unit(u):
        v = u - 8
        w = v % 4
        z = u - 24
        near = u < 8
        far = u >= 24
        fc = jnp.where(near, u // 4, jnp.where(far, z % 2, w // 2))
        part = jnp.where(near, u % 4, jnp.where(far, z // 2, v // 4))
        fy = jnp.where(near, 0, jnp.where(far, 1, w % 2))
        fx = jnp.where(near, 0, jnp.where(far, 1, 1 - w % 2))
        return place.at(fx, fy, fc), part

    def project_phase(w_v, h_v):
        def x_piece(p):
            return pltpu.make_async_copy(x_ref.at[pl.ds(p * PIECE, PIECE)], h_v.at[1, pl.ds(p % 2 * PIECE, PIECE)], n_sem.at[0, p % 2])

        def h_piece(p):
            return pltpu.make_async_copy(h_v.at[0, pl.ds(p % 2 * PIECE, PIECE)], hbuf.at[place.me, pl.ds(p * PIECE, PIECE)], n_sem.at[1, p % 2])

        x_piece(0).start()
        x_piece(1).start()
        for n, w in enumerate(weights):
            pltpu.make_async_copy(w, w_v.at[n], w_sem.at[n]).start()
        barrier_signal(place, range(7))
        for p in range(PIECES):
            x_piece(p).wait()

            def normalize(r, c, p=p):
                rows = pl.ds(pl.multiple_of(p % 2 * PIECE + r * 16, 16), 16)
                xf = h_v[1, rows, :].astype(F32)
                inv = lax.rsqrt(jnp.mean(xf * xf, axis=-1, keepdims=True) + 1e-5)
                h_v[0, rows, :] = (xf * inv * an_ref[...]).astype(BF16)
                return c

            lax.fori_loop(0, PIECE // 16, normalize, 0)
            h_piece(p).start()
            if p + 2 < PIECES:
                x_piece(p + 2).start()
            h_piece(p).wait()
            if p == 0:
                barrier_wait(7)
            own(p, 0, XN).start()
            own(p, 1, YN).start()
            own(p, 2, SIB).start()

        def load(u, slot):
            block, half = unit(u)
            rows = pl.ds(pl.multiple_of(half * UNIT, UNIT), UNIT)
            return pltpu.make_async_copy(hbuf.at[block, rows], h_v.at[slot], h_sem.at[slot])

        def start_load(u):
            load(u, u % 2).start()

        def step(u, carry):
            slot = u % 2
            for g in range(4):
                @pl.when(u == 8 + 4 * g)
                def _(g=g):
                    for p in (2 * g, 2 * g + 1):
                        arrived(XN, p)
                        arrived(YN, p)
                        for f in forwards(p):
                            relay(*f).start()

                @pl.when(u == 24 + 2 * g)
                def _(g=g):
                    for p in (2 * g, 2 * g + 1):
                        arrived(DG, p)
                        relay(DG, p, 6, SDG, SIB).start()
                    if g == 2:
                        for c in range(EARLY):
                            for half in range(2):
                                wo_part(c, half).start()

            def opens(t):
                return (t == 0) | ((t >= 8) & (t < 24) & (t % 4 == 0)) | ((t >= 24) & (t % 2 == 0))

            @pl.when(opens(u))
            def _():
                start_load(u)

            for g in range(4):
                for nxt, kind in ((4 + g, SIB), (10 + 4 * g, SX), (11 + 4 * g, SY), (25 + 2 * g, SDG)):
                    @pl.when(u + 1 == nxt)
                    def _(kind=kind, g=g):
                        arrived(kind, 2 * g)
                        arrived(kind, 2 * g + 1)

            @pl.when((u + 1 < 32) & jnp.logical_not(opens(u + 1)))
            def _():
                start_load(u + 1)

            @pl.when(u == 0)
            def _():
                for n, w in enumerate(weights):
                    pltpu.make_async_copy(w, w_v.at[n], w_sem.at[n]).wait()

            load(u, slot).wait()
            block, half = unit(u)
            rows = pl.ds(pl.multiple_of(block * BLOCK + half * UNIT, UNIT), UNIT)

            def part(n, c):
                r = jnp.dot(h_v[slot], w_v[n], preferred_element_type=F32).astype(BF16)
                for m in range(3):
                    @pl.when(n == m)
                    def _(m=m):
                        for h in range(HEADS):
                            qkv[m][h, rows, :] = r[:, h * HEAD_DIM:(h + 1) * HEAD_DIM]

                @pl.when(n < 2)
                def _():
                    rf = r.astype(F32)
                    col = jnp.sum(rf * rf, axis=1, keepdims=True)
                    for b in range(UNIT // 128):
                        row = jnp.sum(jnp.where(eye, col[b * 128:(b + 1) * 128], 0.0), axis=0, keepdims=True)
                        ssq_v[pl.ds(block * 8 + n * 4 + half, 1), :] = row
                return c

            lax.fori_loop(0, 3, part, 0)
            return carry

        lax.fori_loop(0, 32, step, 0)

    pl.run_scoped(project_phase, pltpu.VMEM((3, WIDTH, COLS), BF16), pltpu.VMEM((2, UNIT, WIDTH), BF16))

    for k in range(7):
        share(k).start()
    mine = pltpu.make_async_copy(ssq_v, ssq_all.at[place.me], ss_loc)
    mine.start()
    for c in range(EARLY, WO_PARTS):
        for half in range(2):
            wo_part(c, half).start()

    def to_sib(ysend, s):
        return remote(ysend, recv0.at[s % 2], y_send, y_recv.at[s % 2], SIB)

    def hop(s1, s, half):
        b = s % 2
        return remote(s1.at[b, half], r1.at[s % 4, half], s1_send.at[b, half], s1_recv.at[s % 4, half], (YN, XN)[half])

    def o_part(o_v, s, half, n):
        chip = place.at(*((1, 0, 0), (0, 1, 0))[half]) // 2 if n == 0 else place.at(1, 1, 0) // 2
        rows = pl.ds(pl.multiple_of(chip * 2 * ROWS, 2 * ROWS), 2 * ROWS)
        return remote(o_v.at[s, rows], o_in.at[half, s, n], o_send.at[half, s, n], o_recv.at[half, s, n], (XN, YN)[half])

    def attend_phase(wo_v, o_v, tab_v, ysend, yown, s1, keep, x_v):
        tab = pltpu.make_async_copy(tab_ref, tab_v, tab_sem)
        tab.start()

        def wo_load(half):
            return pltpu.make_async_copy(wo_ref.at[:, pl.ds(half * HALF, HALF)], wo_v.at[half], wo_sem.at[half])

        for half in range(2):
            wo_load(half).start()
        mine.wait()
        for k in range(7):
            shared(k).wait_recv()
        tab.wait()
        low = lax.broadcasted_iota(jnp.int32, (128, 128), 1) < 64
        gains = [[g[h * HEAD_DIM:(h + 1) * HEAD_DIM][None] for h in range(HEADS)] for g in (qg_ref, kg_ref)]

        def rotate(g, carry):
            rows = pl.ds(pl.multiple_of(g * 128, 128), 128)
            t = tab_v[rows, :]
            turned = pltpu.roll(t, 64, 1)
            cos = jnp.where(low, t, turned)
            sin = jnp.where(low, -turned, t)
            for n in range(2):
                at = g // 4 * 8 + n * 4 + g % 4
                total = jnp.sum(ssq_all[:, pl.ds(at, 1), :], axis=0)
                col = jnp.sum(jnp.where(eye, total, 0.0), axis=1, keepdims=True)
                inv = lax.rsqrt(col / WIDTH + 1e-5)
                for h in range(HEADS):
                    x = qkv[n][h, rows, :].astype(F32) * inv * gains[n][h]
                    qkv[n][h, rows, :] = (x * cos + pltpu.roll(x, 64, 1) * sin).astype(BF16)
            return carry

        lax.fori_loop(0, SEQ // 128, rotate, 0, unroll=2)

        def x_load(s):
            return pltpu.make_async_copy(x_ref.at[pl.ds(pl.multiple_of(s * ROWS, ROWS), ROWS)], x_v, x_sem)

        def tiles(body):
            def run(t, c):
                body(pl.ds(pl.multiple_of(t * TILE, TILE), TILE), t)
                return c
            lax.fori_loop(0, HALF // TILE, run, 0)

        def operand(s, half):
            rows = []
            for fc in (1, 0):
                for n, far in enumerate(((0, 0), ((0, 1), (1, 0))[half])):
                    d = place.at(far[0], far[1], fc)
                    mine_o = o_v[s, pl.ds(pl.multiple_of(d * ROWS, ROWS), ROWS), :]
                    theirs = o_in[half, s, n, pl.ds(pl.multiple_of(d % 2 * ROWS, ROWS), ROWS), :]
                    rows.append(jnp.concatenate([mine_o, theirs], axis=1))
            return jnp.concatenate(rows, axis=0)

        def stage_b(s):
            @pl.when(s == 0)
            def _():
                for half in range(2):
                    wo_load(half).wait()
                    for c in range(WO_PARTS):
                        wo_part(c, half).wait_recv()

            @pl.when(s >= 1)
            def _():
                to_sib(ysend, s - 1).wait_send()

            for half in range(2):
                for n in range(2):
                    o_part(o_v, s, half, n).wait_recv()
                rows = operand(s, half)

                def body(cols, t, half=half, rows=rows):
                    w = jnp.concatenate([wo_v[half, :, cols], wr[half, :, cols]], axis=0)
                    y = jnp.dot(rows, w, preferred_element_type=F32)
                    ysend[half, :, cols] = y[:2 * ROWS].astype(BF16)
                    yown[half, :, cols] = y[2 * ROWS:]
                tiles(body)
            to_sib(ysend, s).start()

        def stage_c(s):
            b = s % 2
            to_sib(ysend, s).wait_recv()

            @pl.when(s >= 2)
            def _():
                for half in range(2):
                    hop(s1, s - 2, half).wait_send()

            for half in range(2):
                def body(cols, t, half=half):
                    y = yown[half, :, cols] + recv0[b, half, :, cols].astype(F32)
                    keep[b, half, :, cols] = y[:ROWS]
                    s1[b, half, :, cols] = y[ROWS:].astype(BF16)
                tiles(body)
                hop(s1, s, half).start()

        def stage_d(s):
            b = s % 2
            x_load(s).wait()

            for half in range(2):
                hop(s1, s, half).wait_recv()

                def body(cols, t, half=half):
                    y = (keep[b, half, :, cols] + r1[s % 4, half, :, cols].astype(F32)).astype(BF16).astype(F32)
                    whole = pl.ds(pl.multiple_of(half * HALF + t * TILE, TILE), TILE)
                    out_ref[pl.ds(pl.multiple_of(s * ROWS, ROWS), ROWS), whole] = (x_v[:, whole].astype(F32) + y).astype(BF16)
                tiles(body)

        def attend(i, h):
            q = jnp.concatenate([q_ref[h, pl.ds(pl.multiple_of(d * BLOCK + i * ROWS, ROWS), ROWS), :] for d in range(TP)], axis=0)
            dims = (((1,), (1,)), ((), ()))

            def scores(j):
                return lax.dot_general(q[j * ROWS:], k_ref[h, j * BLOCK:(j + 1) * BLOCK, :], dims, preferred_element_type=F32)

            row = lax.broadcasted_iota(jnp.int32, (ROWS, BLOCK), 0) + i * ROWS
            keep_mask = lax.broadcasted_iota(jnp.int32, (ROWS, BLOCK), 1) <= row
            m = l = acc = None
            ahead = scores(0)
            for j in range(TP):
                s = ahead
                if j + 1 < TP:
                    ahead = scores(j + 1)
                top = jnp.where(keep_mask, s[:ROWS], -1e30)
                s = top if j == TP - 1 else jnp.concatenate([top, s[ROWS:]], axis=0)
                peak = jnp.max(s, axis=1, keepdims=True) * scale
                new_m = peak if j == 0 else jnp.maximum(m, peak)
                p = jnp.exp2(s * scale - new_m)
                part = p[:, 0:128]
                for c in range(1, BLOCK // 128):
                    part = part + p[:, c * 128:(c + 1) * 128]
                pv = jnp.dot(p.astype(BF16), v_ref[h, j * BLOCK:(j + 1) * BLOCK, :], preferred_element_type=F32)
                if j == 0:
                    l, acc = part, pv
                else:
                    alpha = jnp.exp2(m - new_m)
                    l = l * alpha + part
                    acc = acc * alpha + pv
                total = jnp.sum(l[:ROWS], axis=1, keepdims=True)
                o_v[i, j * ROWS:(j + 1) * ROWS, pl.ds(pl.multiple_of(h * HEAD_DIM, HEAD_DIM), HEAD_DIM)] = (
                    acc[:ROWS] / total).astype(BF16)
                if j + 1 < TP:
                    m, l, acc = new_m[ROWS:], l[ROWS:], acc[ROWS:]

        def substep(s):
            @pl.when((s >= 3) & (s < STEPS + 3))
            def _():
                stage_d(s - 3)

            @pl.when((s >= 2) & (s < STEPS + 2))
            def _():
                x_load(s - 2).start()

            @pl.when((s >= 1) & (s <= STEPS))
            def _():
                stage_c(s - 1)

            @pl.when((s >= 0) & (s < STEPS))
            def _():
                stage_b(s)

        def step(i, carry):
            def head(h, z):
                @pl.when(i < STEPS)
                def _():
                    attend(i, h)

                    @pl.when(h == HEADS - 1)
                    def _():
                        for half in range(2):
                            for n in range(2):
                                o_part(o_v, i, half, n).start()

                @pl.when((i >= LAG) & ((h == 1) | (h == HEADS - 1)))
                def _():
                    substep(2 * (i - LAG) + h // (HEADS - 1) - 1)
                return z

            lax.fori_loop(0, HEADS, head, 0)
            return carry

        lax.fori_loop(0, LAG + STEPS // 2 + 2, step, 0)
        to_sib(ysend, STEPS - 1).wait_send()
        for s in (STEPS - 2, STEPS - 1):
            for half in range(2):
                hop(s1, s, half).wait_send()
        for s in range(STEPS):
            for half in range(2):
                for n in range(2):
                    o_part(o_v, s, half, n).wait_send()

    pl.run_scoped(attend_phase,
                  pltpu.VMEM((2, COLS, HALF), BF16),
                  pltpu.VMEM((STEPS, BLOCK, COLS), BF16),
                  pltpu.VMEM((SEQ, 128), F32),
                  pltpu.VMEM((2, 2 * ROWS, HALF), BF16),
                  pltpu.VMEM((2, 2 * ROWS, HALF), F32),
                  pltpu.VMEM((2, 2, ROWS, HALF), BF16),
                  pltpu.VMEM((2, 2, ROWS, HALF), F32),
                  pltpu.VMEM((ROWS, WIDTH), BF16))
    for p in range(PIECES):
        own(p, 0, XN).wait_send()
        own(p, 1, YN).wait_send()
        own(p, 2, SIB).wait_send()
        for f in forwards(p):
            relay(*f).wait_send()
        relay(DG, p, 6, SDG, SIB).wait_send()
    for k in range(7):
        share(k).wait_send()
    for half in range(2):
        for c in range(WO_PARTS):
            wo_part(c, half).wait_send()


def block_call(x, an, wq, wk, wv, qg, kg, wo, table):
    any_spec = pl.BlockSpec(memory_space=pl.ANY)
    vmem_spec = pl.BlockSpec(memory_space=pltpu.VMEM)
    dma = pltpu.SemaphoreType.DMA
    return pl.pallas_call(
        block_kernel,
        out_shape=[pltpu.VMEM((BLOCK, WIDTH), BF16),
                   pltpu.VMEM((HEADS, SEQ, HEAD_DIM), BF16),
                   pltpu.VMEM((HEADS, SEQ, HEAD_DIM), BF16),
                   jax.ShapeDtypeStruct((TP, BLOCK, WIDTH), BF16)],
        in_specs=[any_spec, vmem_spec, any_spec, any_spec, any_spec, vmem_spec, vmem_spec, any_spec, any_spec],
        out_specs=[vmem_spec] * 3 + [any_spec],
        scratch_shapes=[
            pltpu.VMEM((HEADS, SEQ, HEAD_DIM), BF16),
            pltpu.VMEM((64, 128), F32),
            pltpu.VMEM((TP, 64, 128), F32),
            pltpu.VMEM((2, COLS, HALF), BF16),
            pltpu.VMEM((2, STEPS, 2, 2 * ROWS, COLS), BF16),
            pltpu.VMEM((2, 2, 2 * ROWS, HALF), BF16),
            pltpu.VMEM((4, 2, ROWS, HALF), BF16),
            dma((3,)), dma((2,)), dma((2, 2)), dma((7, PIECES)), dma((7, PIECES)), dma((7,)), dma((7,)), dma(()),
            dma((2, WO_PARTS)), dma((2, WO_PARTS)), dma((2,)), dma(()),
            dma((2, STEPS, 2)), dma((2, STEPS, 2)), dma(()),
            dma(()), dma((2,)), dma((2, 2)), dma((4, 2)),
        ],
        compiler_params=pltpu.CompilerParams(collective_id=0, has_side_effects=True, vmem_limit_bytes=48 * 2**20),
        name="block",
    )(x, an, wq, wk, wv, qg, kg, wo, table)


def rope_table():
    half = HEAD_DIM // 2
    freq = (10000.0 ** (-np.arange(half, dtype=np.float64) * (2.0 / HEAD_DIM))).astype(np.float32)
    angle = (np.arange(SEQ, dtype=np.float32)[:, None] * freq[None, :]).astype(np.float64)
    return np.concatenate([np.cos(angle), np.sin(angle)], axis=1).astype(np.float32)


def solution(mesh):
    table = rope_table()

    def local_block(x_local, attn_gain, wq, wk, wv, q_gain, k_gain, wo):
        out, k, v, _ = block_call(x_local[0], attn_gain[None], wq, wk, wv, q_gain, k_gain, wo, jnp.asarray(table))
        k_cache = jnp.transpose(k, (1, 0, 2))[None]
        v_cache = jnp.transpose(v, (1, 0, 2))[None]
        return out[None], k_cache, v_cache

    seq_spec = P("dp", "tp", None)
    head_spec = P("dp", None, "tp", None)
    col_spec = P(None, "tp")
    return jax.shard_map(local_block, mesh=mesh,
                         in_specs=(seq_spec, P(None), col_spec, col_spec, col_spec, P("tp"), P("tp"), P("tp", None)),
                         out_specs=(seq_spec, head_spec, head_spec), check_vma=False)
```

```python
import functools

import jax
import jax.numpy as jnp
import numpy as np
from jax import lax
from jax.experimental import pallas as pl
from jax.experimental.pallas import tpu as pltpu
from jax.sharding import PartitionSpec as P

MESH = pl.DeviceIdType.MESH
HEAD_DIM = 128
HEADS = 5
COLS = HEADS * HEAD_DIM
WIDTH = 5120
BLOCK = 512
TP = 8
SEQ = TP * BLOCK
PIECES = 8
PIECE = BLOCK // PIECES
UNIT = 128
STEPS = 8
ROWS = BLOCK // STEPS
HALF = WIDTH // 2
TILE = 512
LAG = 4
EARLY = 1
WO_PARTS = 5
WO_ROWS = COLS // WO_PARTS
F32 = jnp.float32
BF16 = jnp.bfloat16
SIB, XN, YN, DG, SX, SY, SDG = range(7)


class Place:
    def __init__(self):
        me = lax.axis_index("tp")
        self.dp = lax.axis_index("dp")
        self.me = me
        self.core = me % 2
        self.x = (me // 2) % 2
        self.y = me // 4

    def at(self, fx, fy, fc):
        x = self.x + fx * (1 - 2 * self.x)
        y = self.y + fy * (1 - 2 * self.y)
        c = self.core + fc * (1 - 2 * self.core)
        return (y * 2 + x) * 2 + c

    def kind(self, k):
        fx, fy, fc = ((0, 0, 1), (1, 0, 0), (0, 1, 0), (1, 1, 0), (1, 0, 1), (0, 1, 1), (1, 1, 1))[k]
        return self.at(fx, fy, fc)

    def dev(self, index):
        return (self.dp, index)


def barrier_signal(place, kinds):
    for k in kinds:
        pl.semaphore_signal(pltpu.get_barrier_semaphore(), inc=1, device_id=place.dev(place.kind(k)), device_id_type=MESH)


def barrier_wait(count):
    pl.semaphore_wait(pltpu.get_barrier_semaphore(), count)


def diagonal():
    r = lax.broadcasted_iota(jnp.int32, (128, 128), 0)
    c = lax.broadcasted_iota(jnp.int32, (128, 128), 1)
    return r == c


def block_kernel(x_ref, an_ref, wq_ref, wk_ref, wv_ref, qg_ref, kg_ref, wo_ref, tab_ref, out_ref, k_ref, v_ref, hbuf,
                 q_ref, ssq_v, ssq_all, wr, o_in, recv0, r1,
                 w_sem, h_sem, n_sem, send_sem, recv_sem, ss_send, ss_recv, ss_loc,
                 wo_send, wo_recv, wo_sem, tab_sem, o_send, o_recv, x_sem, y_send, y_recv, s1_send, s1_recv):
    place = Place()
    scale = float(HEAD_DIM ** -0.5 * np.log2(np.e))
    eye = diagonal()
    weights = (wq_ref, wk_ref, wv_ref)

    def remote(src, dst, send, recv, kind):
        return pltpu.make_async_remote_copy(src_ref=src, dst_ref=dst, send_sem=send, recv_sem=recv,
                                            device_id=place.dev(place.kind(kind)), device_id_type=MESH)

    def copy(src_ref, block, p, send, kind, target):
        return remote(src_ref, hbuf.at[block, pl.ds(p * PIECE, PIECE)], send_sem.at[send, p], recv_sem.at[kind, p], target)

    def own(p, send, kind):
        return copy(hbuf.at[place.me, pl.ds(p * PIECE, PIECE)], place.me, p, send, kind, kind)

    def relay(owner, p, send, kind, target):
        block = place.kind(owner)
        return copy(hbuf.at[block, pl.ds(p * PIECE, PIECE)], block, p, send, kind, target)

    def arrived(kind, p):
        relay(kind, p, 0, kind, SIB).wait_recv()

    def forwards(p):
        out = [(XN, p, 3, SX, SIB), (YN, p, 4, SY, SIB)]
        out.append((XN, p, 5, DG, YN) if p % 2 == 0 else (YN, p, 5, DG, XN))
        return out

    def wo_part(c, half):
        rows = pl.ds(c * WO_ROWS, WO_ROWS)
        return remote(wo_ref.at[rows, pl.ds(half * HALF, HALF)], wr.at[half, rows],
                      wo_send.at[half, c], wo_recv.at[half, c], (XN, YN)[half])

    def share(k):
        return remote(ssq_v, ssq_all.at[place.me], ss_send.at[k], ss_recv.at[k], k)

    def shared(k):
        return remote(ssq_v, ssq_all.at[place.kind(k)], ss_send.at[k], ss_recv.at[k], k)

    qkv = (q_ref, k_ref, v_ref)

    def unit(u):
        v = u - 8
        w = v % 4
        z = u - 24
        near = u < 8
        far = u >= 24
        fc = jnp.where(near, u // 4, jnp.where(far, z % 2, w // 2))
        part = jnp.where(near, u % 4, jnp.where(far, z // 2, v // 4))
        fy = jnp.where(near, 0, jnp.where(far, 1, w % 2))
        fx = jnp.where(near, 0, jnp.where(far, 1, 1 - w % 2))
        return place.at(fx, fy, fc), part

    def project_phase(w_v, h_v):
        def x_piece(p):
            return pltpu.make_async_copy(x_ref.at[pl.ds(p * PIECE, PIECE)], h_v.at[1, pl.ds(p % 2 * PIECE, PIECE)], n_sem.at[0, p % 2])

        def h_piece(p):
            return pltpu.make_async_copy(h_v.at[0, pl.ds(p % 2 * PIECE, PIECE)], hbuf.at[place.me, pl.ds(p * PIECE, PIECE)], n_sem.at[1, p % 2])

        x_piece(0).start()
        x_piece(1).start()
        for n, w in enumerate(weights):
            pltpu.make_async_copy(w, w_v.at[n], w_sem.at[n]).start()
        barrier_signal(place, range(7))
        for p in range(PIECES):
            x_piece(p).wait()

            def normalize(r, c, p=p):
                rows = pl.ds(pl.multiple_of(p % 2 * PIECE + r * 16, 16), 16)
                xf = h_v[1, rows, :].astype(F32)
                inv = lax.rsqrt(jnp.mean(xf * xf, axis=-1, keepdims=True) + 1e-5)
                h_v[0, rows, :] = (xf * inv * an_ref[...]).astype(BF16)
                return c

            lax.fori_loop(0, PIECE // 16, normalize, 0)
            h_piece(p).start()
            if p + 2 < PIECES:
                x_piece(p + 2).start()
            h_piece(p).wait()
            if p == 0:
                barrier_wait(7)
            own(p, 0, XN).start()
            own(p, 1, YN).start()
            own(p, 2, SIB).start()

        def load(u, slot):
            block, half = unit(u)
            rows = pl.ds(pl.multiple_of(half * UNIT, UNIT), UNIT)
            return pltpu.make_async_copy(hbuf.at[block, rows], h_v.at[slot], h_sem.at[slot])

        def start_load(u):
            load(u, u % 2).start()

        def step(u, carry):
            slot = u % 2
            for g in range(4):
                @pl.when(u == 8 + 4 * g)
                def _(g=g):
                    for p in (2 * g, 2 * g + 1):
                        arrived(XN, p)
                        arrived(YN, p)
                        for f in forwards(p):
                            relay(*f).start()

                @pl.when(u == 24 + 2 * g)
                def _(g=g):
                    for p in (2 * g, 2 * g + 1):
                        arrived(DG, p)
                        relay(DG, p, 6, SDG, SIB).start()
                    if g == 2:
                        for c in range(EARLY):
                            for half in range(2):
                                wo_part(c, half).start()

            def opens(t):
                return (t == 0) | ((t >= 8) & (t < 24) & (t % 4 == 0)) | ((t >= 24) & (t % 2 == 0))

            @pl.when(opens(u))
            def _():
                start_load(u)

            for g in range(4):
                for nxt, kind in ((4 + g, SIB), (10 + 4 * g, SX), (11 + 4 * g, SY), (25 + 2 * g, SDG)):
                    @pl.when(u + 1 == nxt)
                    def _(kind=kind, g=g):
                        arrived(kind, 2 * g)
                        arrived(kind, 2 * g + 1)

            @pl.when((u + 1 < 32) & jnp.logical_not(opens(u + 1)))
            def _():
                start_load(u + 1)

            @pl.when(u == 0)
            def _():
                for n, w in enumerate(weights):
                    pltpu.make_async_copy(w, w_v.at[n], w_sem.at[n]).wait()

            load(u, slot).wait()
            block, half = unit(u)
            rows = pl.ds(pl.multiple_of(block * BLOCK + half * UNIT, UNIT), UNIT)

            def part(n, c):
                r = jnp.dot(h_v[slot], w_v[n], preferred_element_type=F32).astype(BF16)
                for m in range(3):
                    @pl.when(n == m)
                    def _(m=m):
                        for h in range(HEADS):
                            qkv[m][h, rows, :] = r[:, h * HEAD_DIM:(h + 1) * HEAD_DIM]

                @pl.when(n < 2)
                def _():
                    rf = r.astype(F32)
                    col = jnp.sum(rf * rf, axis=1, keepdims=True)
                    for b in range(UNIT // 128):
                        row = jnp.sum(jnp.where(eye, col[b * 128:(b + 1) * 128], 0.0), axis=0, keepdims=True)
                        ssq_v[pl.ds(block * 8 + n * 4 + half, 1), :] = row
                return c

            lax.fori_loop(0, 3, part, 0)
            return carry

        lax.fori_loop(0, 32, step, 0)

    pl.run_scoped(project_phase, pltpu.VMEM((3, WIDTH, COLS), BF16), pltpu.VMEM((2, UNIT, WIDTH), BF16))

    for k in range(7):
        share(k).start()
    mine = pltpu.make_async_copy(ssq_v, ssq_all.at[place.me], ss_loc)
    mine.start()
    for c in range(EARLY, WO_PARTS):
        for half in range(2):
            wo_part(c, half).start()

    def to_sib(ysend, s):
        return remote(ysend, recv0.at[s % 2], y_send, y_recv.at[s % 2], SIB)

    def hop(s1, s, half):
        b = s % 2
        return remote(s1.at[b, half], r1.at[s % 4, half], s1_send.at[b, half], s1_recv.at[s % 4, half], (YN, XN)[half])

    def o_part(o_v, s, half, n):
        chip = place.at(*((1, 0, 0), (0, 1, 0))[half]) // 2 if n == 0 else place.at(1, 1, 0) // 2
        rows = pl.ds(pl.multiple_of(chip * 2 * ROWS, 2 * ROWS), 2 * ROWS)
        return remote(o_v.at[s, rows], o_in.at[half, s, n], o_send.at[half, s, n], o_recv.at[half, s, n], (XN, YN)[half])

    def attend_phase(wo_v, o_v, tab_v, ysend, yown, s1, keep, x_v):
        tab = pltpu.make_async_copy(tab_ref, tab_v, tab_sem)
        tab.start()

        def wo_load(half):
            return pltpu.make_async_copy(wo_ref.at[:, pl.ds(half * HALF, HALF)], wo_v.at[half], wo_sem.at[half])

        for half in range(2):
            wo_load(half).start()
        mine.wait()
        for k in range(7):
            shared(k).wait_recv()
        tab.wait()
        low = lax.broadcasted_iota(jnp.int32, (128, 128), 1) < 64
        gains = [[g[h * HEAD_DIM:(h + 1) * HEAD_DIM][None] for h in range(HEADS)] for g in (qg_ref, kg_ref)]

        def rotate(g, carry):
            rows = pl.ds(pl.multiple_of(g * 128, 128), 128)
            t = tab_v[rows, :]
            turned = pltpu.roll(t, 64, 1)
            cos = jnp.where(low, t, turned)
            sin = jnp.where(low, -turned, t)
            for n in range(2):
                at = g // 4 * 8 + n * 4 + g % 4
                total = jnp.sum(ssq_all[:, pl.ds(at, 1), :], axis=0)
                col = jnp.sum(jnp.where(eye, total, 0.0), axis=1, keepdims=True)
                inv = lax.rsqrt(col / WIDTH + 1e-5)
                for h in range(HEADS):
                    x = qkv[n][h, rows, :].astype(F32) * inv * gains[n][h]
                    qkv[n][h, rows, :] = (x * cos + pltpu.roll(x, 64, 1) * sin).astype(BF16)
            return carry

        lax.fori_loop(0, SEQ // 128, rotate, 0, unroll=2)

        def x_load(s):
            return pltpu.make_async_copy(x_ref.at[pl.ds(pl.multiple_of(s * ROWS, ROWS), ROWS)], x_v, x_sem)

        def tiles(body):
            def run(t, c):
                body(pl.ds(pl.multiple_of(t * TILE, TILE), TILE), t)
                return c
            lax.fori_loop(0, HALF // TILE, run, 0)

        def operand(s, half):
            rows = []
            for fc in (1, 0):
                for n, far in enumerate(((0, 0), ((0, 1), (1, 0))[half])):
                    d = place.at(far[0], far[1], fc)
                    mine_o = o_v[s, pl.ds(pl.multiple_of(d * ROWS, ROWS), ROWS), :]
                    theirs = o_in[half, s, n, pl.ds(pl.multiple_of(d % 2 * ROWS, ROWS), ROWS), :]
                    rows.append(jnp.concatenate([mine_o, theirs], axis=1))
            return jnp.concatenate(rows, axis=0)

        def stage_b(s):
            @pl.when(s == 0)
            def _():
                for half in range(2):
                    wo_load(half).wait()
                    for c in range(WO_PARTS):
                        wo_part(c, half).wait_recv()

            @pl.when(s >= 1)
            def _():
                to_sib(ysend, s - 1).wait_send()

            for half in range(2):
                for n in range(2):
                    o_part(o_v, s, half, n).wait_recv()
                rows = operand(s, half)

                def body(cols, t, half=half, rows=rows):
                    w = jnp.concatenate([wo_v[half, :, cols], wr[half, :, cols]], axis=0)
                    y = jnp.dot(rows, w, preferred_element_type=F32)
                    ysend[half, :, cols] = y[:2 * ROWS].astype(BF16)
                    yown[half, :, cols] = y[2 * ROWS:]
                tiles(body)
            to_sib(ysend, s).start()

        def stage_c(s):
            b = s % 2
            to_sib(ysend, s).wait_recv()

            @pl.when(s >= 2)
            def _():
                for half in range(2):
                    hop(s1, s - 2, half).wait_send()

            for half in range(2):
                def body(cols, t, half=half):
                    y = yown[half, :, cols] + recv0[b, half, :, cols].astype(F32)
                    keep[b, half, :, cols] = y[:ROWS]
                    s1[b, half, :, cols] = y[ROWS:].astype(BF16)
                tiles(body)
                hop(s1, s, half).start()

        def stage_d(s):
            b = s % 2
            x_load(s).wait()

            for half in range(2):
                hop(s1, s, half).wait_recv()

                def body(cols, t, half=half):
                    y = (keep[b, half, :, cols] + r1[s % 4, half, :, cols].astype(F32)).astype(BF16).astype(F32)
                    whole = pl.ds(pl.multiple_of(half * HALF + t * TILE, TILE), TILE)
                    out_ref[pl.ds(pl.multiple_of(s * ROWS, ROWS), ROWS), whole] = (x_v[:, whole].astype(F32) + y).astype(BF16)
                tiles(body)

        def attend(i, h):
            q = jnp.concatenate([q_ref[h, pl.ds(pl.multiple_of(d * BLOCK + i * ROWS, ROWS), ROWS), :] for d in range(TP)], axis=0)
            dims = (((1,), (1,)), ((), ()))

            def scores(j):
                return lax.dot_general(q[j * ROWS:], k_ref[h, j * BLOCK:(j + 1) * BLOCK, :], dims, preferred_element_type=F32)

            row = lax.broadcasted_iota(jnp.int32, (ROWS, BLOCK), 0) + i * ROWS
            keep_mask = lax.broadcasted_iota(jnp.int32, (ROWS, BLOCK), 1) <= row
            m = l = acc = None
            ahead = scores(0)
            for j in range(TP):
                s = ahead
                if j + 1 < TP:
                    ahead = scores(j + 1)
                top = jnp.where(keep_mask, s[:ROWS], -1e30)
                s = top if j == TP - 1 else jnp.concatenate([top, s[ROWS:]], axis=0)
                peak = jnp.max(s, axis=1, keepdims=True) * scale
                new_m = peak if j == 0 else jnp.maximum(m, peak)
                p = jnp.exp2(s * scale - new_m)
                part = p[:, 0:128]
                for c in range(1, BLOCK // 128):
                    part = part + p[:, c * 128:(c + 1) * 128]
                pv = jnp.dot(p.astype(BF16), v_ref[h, j * BLOCK:(j + 1) * BLOCK, :], preferred_element_type=F32)
                if j == 0:
                    l, acc = part, pv
                else:
                    alpha = jnp.exp2(m - new_m)
                    l = l * alpha + part
                    acc = acc * alpha + pv
                total = jnp.sum(l[:ROWS], axis=1, keepdims=True)
                o_v[i, j * ROWS:(j + 1) * ROWS, pl.ds(pl.multiple_of(h * HEAD_DIM, HEAD_DIM), HEAD_DIM)] = (
                    acc[:ROWS] / total).astype(BF16)
                if j + 1 < TP:
                    m, l, acc = new_m[ROWS:], l[ROWS:], acc[ROWS:]

        def substep(s):
            @pl.when((s >= 3) & (s < STEPS + 3))
            def _():
                stage_d(s - 3)

            @pl.when((s >= 2) & (s < STEPS + 2))
            def _():
                x_load(s - 2).start()

            @pl.when((s >= 1) & (s <= STEPS))
            def _():
                stage_c(s - 1)

            @pl.when((s >= 0) & (s < STEPS))
            def _():
                stage_b(s)

        def step(i, carry):
            def head(h, z):
                @pl.when(i < STEPS)
                def _():
                    attend(i, h)

                    @pl.when(h == HEADS - 1)
                    def _():
                        for half in range(2):
                            for n in range(2):
                                o_part(o_v, i, half, n).start()

                @pl.when((i >= LAG) & ((h == 1) | (h == HEADS - 1)))
                def _():
                    substep(2 * (i - LAG) + h // (HEADS - 1) - 1)
                return z

            lax.fori_loop(0, HEADS, head, 0)
            return carry

        lax.fori_loop(0, LAG + STEPS // 2 + 2, step, 0)
        to_sib(ysend, STEPS - 1).wait_send()
        for s in (STEPS - 2, STEPS - 1):
            for half in range(2):
                hop(s1, s, half).wait_send()
        for s in range(STEPS):
            for half in range(2):
                for n in range(2):
                    o_part(o_v, s, half, n).wait_send()

    pl.run_scoped(attend_phase,
                  pltpu.VMEM((2, COLS, HALF), BF16),
                  pltpu.VMEM((STEPS, BLOCK, COLS), BF16),
                  pltpu.VMEM((SEQ, 128), F32),
                  pltpu.VMEM((2, 2 * ROWS, HALF), BF16),
                  pltpu.VMEM((2, 2 * ROWS, HALF), F32),
                  pltpu.VMEM((2, 2, ROWS, HALF), BF16),
                  pltpu.VMEM((2, 2, ROWS, HALF), F32),
                  pltpu.VMEM((ROWS, WIDTH), BF16))
    for p in range(PIECES):
        own(p, 0, XN).wait_send()
        own(p, 1, YN).wait_send()
        own(p, 2, SIB).wait_send()
        for f in forwards(p):
            relay(*f).wait_send()
        relay(DG, p, 6, SDG, SIB).wait_send()
    for k in range(7):
        share(k).wait_send()
    for half in range(2):
        for c in range(WO_PARTS):
            wo_part(c, half).wait_send()


def block_call(x, an, wq, wk, wv, qg, kg, wo, table):
    any_spec = pl.BlockSpec(memory_space=pl.ANY)
    vmem_spec = pl.BlockSpec(memory_space=pltpu.VMEM)
    dma = pltpu.SemaphoreType.DMA
    return pl.pallas_call(
        block_kernel,
        out_shape=[pltpu.VMEM((BLOCK, WIDTH), BF16),
                   pltpu.VMEM((HEADS, SEQ, HEAD_DIM), BF16),
                   pltpu.VMEM((HEADS, SEQ, HEAD_DIM), BF16),
                   jax.ShapeDtypeStruct((TP, BLOCK, WIDTH), BF16)],
        in_specs=[any_spec, vmem_spec, any_spec, any_spec, any_spec, vmem_spec, vmem_spec, any_spec, any_spec],
        out_specs=[vmem_spec] * 3 + [any_spec],
        scratch_shapes=[
            pltpu.VMEM((HEADS, SEQ, HEAD_DIM), BF16),
            pltpu.VMEM((64, 128), F32),
            pltpu.VMEM((TP, 64, 128), F32),
            pltpu.VMEM((2, COLS, HALF), BF16),
            pltpu.VMEM((2, STEPS, 2, 2 * ROWS, COLS), BF16),
            pltpu.VMEM((2, 2, 2 * ROWS, HALF), BF16),
            pltpu.VMEM((4, 2, ROWS, HALF), BF16),
            dma((3,)), dma((2,)), dma((2, 2)), dma((7, PIECES)), dma((7, PIECES)), dma((7,)), dma((7,)), dma(()),
            dma((2, WO_PARTS)), dma((2, WO_PARTS)), dma((2,)), dma(()),
            dma((2, STEPS, 2)), dma((2, STEPS, 2)), dma(()),
            dma(()), dma((2,)), dma((2, 2)), dma((4, 2)),
        ],
        compiler_params=pltpu.CompilerParams(collective_id=0, has_side_effects=True, vmem_limit_bytes=48 * 2**20),
        name="block",
    )(x, an, wq, wk, wv, qg, kg, wo, table)


def write_out(*refs):
    srcs, dsts, sems = refs[:3], refs[3:6], refs[6]
    parts = 4
    copies = []
    for n, (src, dst) in enumerate(zip(srcs, dsts)):
        size = src.shape[-2] // parts
        for p in range(parts):
            at = (slice(None),) * (len(src.shape) - 2) + (pl.ds(p * size, size),)
            copies.append(pltpu.make_async_copy(src.at[at], dst.at[at], sems.at[n, p]))
    for c in copies:
        c.start()
    for c in copies:
        c.wait()


def write_out_call(*arrays):
    return pl.pallas_call(
        write_out,
        out_shape=[jax.ShapeDtypeStruct(a.shape, a.dtype) for a in arrays],
        in_specs=[pl.BlockSpec(memory_space=pltpu.VMEM)] * 3,
        out_specs=[pl.BlockSpec(memory_space=pl.ANY)] * 3,
        scratch_shapes=[pltpu.SemaphoreType.DMA((3, 4))],
        compiler_params=pltpu.CompilerParams(vmem_limit_bytes=2**20),
        name="write_out",
    )(*[pltpu.with_memory_space_constraint(a, pltpu.VMEM) for a in arrays])


def rope_table():
    half = HEAD_DIM // 2
    freq = (10000.0 ** (-np.arange(half, dtype=np.float64) * (2.0 / HEAD_DIM))).astype(np.float32)
    angle = (np.arange(SEQ, dtype=np.float32)[:, None] * freq[None, :]).astype(np.float64)
    return np.concatenate([np.cos(angle), np.sin(angle)], axis=1).astype(np.float32)


def solution(mesh):
    table = rope_table()

    def local_block(x_local, attn_gain, wq, wk, wv, q_gain, k_gain, wo):
        out, k, v, _ = block_call(x_local[0], attn_gain[None], wq, wk, wv, q_gain, k_gain, wo, jnp.asarray(table))
        out, k, v = write_out_call(out, k, v)
        k_cache = jnp.transpose(k, (1, 0, 2))[None]
        v_cache = jnp.transpose(v, (1, 0, 2))[None]
        return out[None], k_cache, v_cache

    seq_spec = P("dp", "tp", None)
    head_spec = P("dp", None, "tp", None)
    col_spec = P(None, "tp")
    return jax.shard_map(local_block, mesh=mesh,
                         in_specs=(seq_spec, P(None), col_spec, col_spec, col_spec, P("tp"), P("tp"), P("tp", None)),
                         out_specs=(seq_spec, head_spec, head_spec), check_vma=False)
```

```python
import functools

import jax
import jax.numpy as jnp
import numpy as np
from jax import lax
from jax.experimental import pallas as pl
from jax.experimental.pallas import tpu as pltpu
from jax.sharding import PartitionSpec as P

MESH = pl.DeviceIdType.MESH
HEAD_DIM = 128
HEADS = 5
COLS = HEADS * HEAD_DIM
WIDTH = 5120
BLOCK = 512
TP = 8
SEQ = TP * BLOCK
PIECES = 8
PIECE = BLOCK // PIECES
UNIT = 128
STEPS = 8
ROWS = BLOCK // STEPS
HALF = WIDTH // 2
TILE = 512
LAG = 4
EARLY = 1
WO_PARTS = 5
WO_ROWS = COLS // WO_PARTS
F32 = jnp.float32
BF16 = jnp.bfloat16
SIB, XN, YN, DG, SX, SY, SDG = range(7)


class Place:
    def __init__(self):
        me = lax.axis_index("tp")
        self.dp = lax.axis_index("dp")
        self.me = me
        self.core = me % 2
        self.x = (me // 2) % 2
        self.y = me // 4

    def at(self, fx, fy, fc):
        x = self.x + fx * (1 - 2 * self.x)
        y = self.y + fy * (1 - 2 * self.y)
        c = self.core + fc * (1 - 2 * self.core)
        return (y * 2 + x) * 2 + c

    def kind(self, k):
        fx, fy, fc = ((0, 0, 1), (1, 0, 0), (0, 1, 0), (1, 1, 0), (1, 0, 1), (0, 1, 1), (1, 1, 1))[k]
        return self.at(fx, fy, fc)

    def dev(self, index):
        return (self.dp, index)


def barrier_signal(place, kinds):
    for k in kinds:
        pl.semaphore_signal(pltpu.get_barrier_semaphore(), inc=1, device_id=place.dev(place.kind(k)), device_id_type=MESH)


def barrier_wait(count):
    pl.semaphore_wait(pltpu.get_barrier_semaphore(), count)


def diagonal():
    r = lax.broadcasted_iota(jnp.int32, (128, 128), 0)
    c = lax.broadcasted_iota(jnp.int32, (128, 128), 1)
    return r == c


def block_kernel(x_ref, an_ref, wq_ref, wk_ref, wv_ref, qg_ref, kg_ref, wo_ref, tab_ref, out_ref, k_ref, v_ref, hbuf,
                 q_ref, ssq_v, ssq_sib, ssq_all, wr, o_in, recv0, r1,
                 w_sem, h_sem, n_sem, send_sem, recv_sem, ss_send, ss_recv,
                 wo_send, wo_recv, wo_sem, tab_sem, o_send, o_recv, x_sem, y_send, y_recv, s1_send, s1_recv):
    place = Place()
    scale = float(HEAD_DIM ** -0.5 * np.log2(np.e))
    eye = diagonal()
    weights = (wq_ref, wk_ref, wv_ref)

    def remote(src, dst, send, recv, kind):
        return pltpu.make_async_remote_copy(src_ref=src, dst_ref=dst, send_sem=send, recv_sem=recv,
                                            device_id=place.dev(place.kind(kind)), device_id_type=MESH)

    def copy(src_ref, block, p, send, kind, target):
        return remote(src_ref, hbuf.at[block, pl.ds(p * PIECE, PIECE)], send_sem.at[send, p], recv_sem.at[kind, p], target)

    def own(p, send, kind):
        return copy(hbuf.at[place.me, pl.ds(p * PIECE, PIECE)], place.me, p, send, kind, kind)

    def relay(owner, p, send, kind, target):
        block = place.kind(owner)
        return copy(hbuf.at[block, pl.ds(p * PIECE, PIECE)], block, p, send, kind, target)

    def arrived(kind, p):
        relay(kind, p, 0, kind, SIB).wait_recv()

    def forwards(p):
        out = [(XN, p, 3, SX, SIB), (YN, p, 4, SY, SIB)]
        out.append((XN, p, 5, DG, YN) if p % 2 == 0 else (YN, p, 5, DG, XN))
        return out

    def wo_part(c, half):
        rows = pl.ds(c * WO_ROWS, WO_ROWS)
        return remote(wo_ref.at[rows, pl.ds(half * HALF, HALF)], wr.at[half, rows],
                      wo_send.at[half, c], wo_recv.at[half, c], (XN, YN)[half])

    def pair():
        return remote(ssq_v, ssq_sib, ss_send.at[SIB], ss_recv.at[SIB], SIB)

    def share(k):
        chip = place.me // 2
        return remote(ssq_all.at[chip], ssq_all.at[chip], ss_send.at[k], ss_recv.at[k], k)

    def shared(k):
        chip = place.kind(k) // 2
        return remote(ssq_all.at[chip], ssq_all.at[chip], ss_send.at[k], ss_recv.at[k], k)

    qkv = (q_ref, k_ref, v_ref)

    def unit(u):
        v = u - 8
        w = v % 4
        z = u - 24
        near = u < 8
        far = u >= 24
        fc = jnp.where(near, u // 4, jnp.where(far, z % 2, w // 2))
        part = jnp.where(near, u % 4, jnp.where(far, z // 2, v // 4))
        fy = jnp.where(near, 0, jnp.where(far, 1, w % 2))
        fx = jnp.where(near, 0, jnp.where(far, 1, 1 - w % 2))
        return place.at(fx, fy, fc), part

    def project_phase(w_v, h_v):
        def x_piece(p):
            return pltpu.make_async_copy(x_ref.at[pl.ds(p * PIECE, PIECE)], h_v.at[1, pl.ds(p % 2 * PIECE, PIECE)], n_sem.at[0, p % 2])

        def h_piece(p):
            return pltpu.make_async_copy(h_v.at[0, pl.ds(p % 2 * PIECE, PIECE)], hbuf.at[place.me, pl.ds(p * PIECE, PIECE)], n_sem.at[1, p % 2])

        x_piece(0).start()
        x_piece(1).start()
        for n, w in enumerate(weights):
            pltpu.make_async_copy(w, w_v.at[n], w_sem.at[n]).start()
        barrier_signal(place, range(7))
        for p in range(PIECES):
            x_piece(p).wait()

            def normalize(r, c, p=p):
                rows = pl.ds(pl.multiple_of(p % 2 * PIECE + r * 16, 16), 16)
                xf = h_v[1, rows, :].astype(F32)
                inv = lax.rsqrt(jnp.mean(xf * xf, axis=-1, keepdims=True) + 1e-5)
                h_v[0, rows, :] = (xf * inv * an_ref[...]).astype(BF16)
                return c

            lax.fori_loop(0, PIECE // 16, normalize, 0)
            h_piece(p).start()
            if p + 2 < PIECES:
                x_piece(p + 2).start()
            h_piece(p).wait()
            if p == 0:
                barrier_wait(7)
            own(p, 0, XN).start()
            own(p, 1, YN).start()
            own(p, 2, SIB).start()

        def load(u, slot):
            block, half = unit(u)
            rows = pl.ds(pl.multiple_of(half * UNIT, UNIT), UNIT)
            return pltpu.make_async_copy(hbuf.at[block, rows], h_v.at[slot], h_sem.at[slot])

        def start_load(u):
            load(u, u % 2).start()

        def step(u, carry):
            slot = u % 2
            for g in range(4):
                @pl.when(u == 8 + 4 * g)
                def _(g=g):
                    for p in (2 * g, 2 * g + 1):
                        arrived(XN, p)
                        arrived(YN, p)
                        for f in forwards(p):
                            relay(*f).start()

                @pl.when(u == 24 + 2 * g)
                def _(g=g):
                    for p in (2 * g, 2 * g + 1):
                        arrived(DG, p)
                        relay(DG, p, 6, SDG, SIB).start()
                    if g == 2:
                        for c in range(EARLY):
                            for half in range(2):
                                wo_part(c, half).start()

            def opens(t):
                return (t == 0) | ((t >= 8) & (t < 24) & (t % 4 == 0)) | ((t >= 24) & (t % 2 == 0))

            @pl.when(opens(u))
            def _():
                start_load(u)

            for g in range(4):
                for nxt, kind in ((4 + g, SIB), (10 + 4 * g, SX), (11 + 4 * g, SY), (25 + 2 * g, SDG)):
                    @pl.when(u + 1 == nxt)
                    def _(kind=kind, g=g):
                        arrived(kind, 2 * g)
                        arrived(kind, 2 * g + 1)

            @pl.when((u + 1 < 32) & jnp.logical_not(opens(u + 1)))
            def _():
                start_load(u + 1)

            @pl.when(u == 0)
            def _():
                for n, w in enumerate(weights):
                    pltpu.make_async_copy(w, w_v.at[n], w_sem.at[n]).wait()

            load(u, slot).wait()
            block, half = unit(u)
            rows = pl.ds(pl.multiple_of(block * BLOCK + half * UNIT, UNIT), UNIT)

            def part(n, c):
                r = jnp.dot(h_v[slot], w_v[n], preferred_element_type=F32).astype(BF16)
                for m in range(3):
                    @pl.when(n == m)
                    def _(m=m):
                        for h in range(HEADS):
                            qkv[m][h, rows, :] = r[:, h * HEAD_DIM:(h + 1) * HEAD_DIM]

                @pl.when(n < 2)
                def _():
                    rf = r.astype(F32)
                    col = jnp.sum(rf * rf, axis=1, keepdims=True)
                    for b in range(UNIT // 128):
                        row = jnp.sum(jnp.where(eye, col[b * 128:(b + 1) * 128], 0.0), axis=0, keepdims=True)
                        ssq_v[pl.ds(block * 8 + n * 4 + half, 1), :] = row
                return c

            lax.fori_loop(0, 3, part, 0)
            return carry

        lax.fori_loop(0, 32, step, 0)

    pl.run_scoped(project_phase, pltpu.VMEM((3, WIDTH, COLS), BF16), pltpu.VMEM((2, UNIT, WIDTH), BF16))

    pair().start()
    pair().wait_recv()
    ssq_all[place.me // 2] = ssq_v[...] + ssq_sib[...]
    for k in (XN, YN, DG):
        share(k).start()
    for c in range(EARLY, WO_PARTS):
        for half in range(2):
            wo_part(c, half).start()

    def to_sib(ysend, s):
        return remote(ysend, recv0.at[s % 2], y_send, y_recv.at[s % 2], SIB)

    def hop(s1, s, half):
        b = s % 2
        return remote(s1.at[b, half], r1.at[s % 4, half], s1_send.at[b, half], s1_recv.at[s % 4, half], (YN, XN)[half])

    def o_part(o_v, s, half, n):
        chip = place.at(*((1, 0, 0), (0, 1, 0))[half]) // 2 if n == 0 else place.at(1, 1, 0) // 2
        rows = pl.ds(pl.multiple_of(chip * 2 * ROWS, 2 * ROWS), 2 * ROWS)
        return remote(o_v.at[s, rows], o_in.at[half, s, n], o_send.at[half, s, n], o_recv.at[half, s, n], (XN, YN)[half])

    def attend_phase(wo_v, o_v, tab_v, ysend, yown, s1, keep, x_v):
        tab = pltpu.make_async_copy(tab_ref, tab_v, tab_sem)
        tab.start()

        def wo_load(half):
            return pltpu.make_async_copy(wo_ref.at[:, pl.ds(half * HALF, HALF)], wo_v.at[half], wo_sem.at[half])

        for half in range(2):
            wo_load(half).start()
        for k in (XN, YN, DG):
            shared(k).wait_recv()
        tab.wait()
        low = lax.broadcasted_iota(jnp.int32, (128, 128), 1) < 64
        gains = [[g[h * HEAD_DIM:(h + 1) * HEAD_DIM][None] for h in range(HEADS)] for g in (qg_ref, kg_ref)]

        def rotate(g, carry):
            rows = pl.ds(pl.multiple_of(g * 128, 128), 128)
            t = tab_v[rows, :]
            turned = pltpu.roll(t, 64, 1)
            cos = jnp.where(low, t, turned)
            sin = jnp.where(low, -turned, t)
            for n in range(2):
                at = g // 4 * 8 + n * 4 + g % 4
                total = jnp.sum(ssq_all[:, pl.ds(at, 1), :], axis=0)
                col = jnp.sum(jnp.where(eye, total, 0.0), axis=1, keepdims=True)
                inv = lax.rsqrt(col / WIDTH + 1e-5)
                for h in range(HEADS):
                    x = qkv[n][h, rows, :].astype(F32) * inv * gains[n][h]
                    qkv[n][h, rows, :] = (x * cos + pltpu.roll(x, 64, 1) * sin).astype(BF16)
            return carry

        lax.fori_loop(0, SEQ // 128, rotate, 0, unroll=2)

        def x_load(s):
            return pltpu.make_async_copy(x_ref.at[pl.ds(pl.multiple_of(s * ROWS, ROWS), ROWS)], x_v, x_sem)

        def tiles(body):
            def run(t, c):
                body(pl.ds(pl.multiple_of(t * TILE, TILE), TILE), t)
                return c
            lax.fori_loop(0, HALF // TILE, run, 0)

        def operand(s, half):
            rows = []
            for fc in (1, 0):
                for n, far in enumerate(((0, 0), ((0, 1), (1, 0))[half])):
                    d = place.at(far[0], far[1], fc)
                    mine_o = o_v[s, pl.ds(pl.multiple_of(d * ROWS, ROWS), ROWS), :]
                    theirs = o_in[half, s, n, pl.ds(pl.multiple_of(d % 2 * ROWS, ROWS), ROWS), :]
                    rows.append(jnp.concatenate([mine_o, theirs], axis=1))
            return jnp.concatenate(rows, axis=0)

        def stage_b(s):
            @pl.when(s == 0)
            def _():
                for half in range(2):
                    wo_load(half).wait()
                    for c in range(WO_PARTS):
                        wo_part(c, half).wait_recv()

            @pl.when(s >= 1)
            def _():
                to_sib(ysend, s - 1).wait_send()

            for half in range(2):
                for n in range(2):
                    o_part(o_v, s, half, n).wait_recv()
                rows = operand(s, half)

                def body(cols, t, half=half, rows=rows):
                    w = jnp.concatenate([wo_v[half, :, cols], wr[half, :, cols]], axis=0)
                    y = jnp.dot(rows, w, preferred_element_type=F32)
                    ysend[half, :, cols] = y[:2 * ROWS].astype(BF16)
                    yown[half, :, cols] = y[2 * ROWS:]
                tiles(body)
            to_sib(ysend, s).start()

        def stage_c(s):
            b = s % 2
            to_sib(ysend, s).wait_recv()

            @pl.when(s >= 2)
            def _():
                for half in range(2):
                    hop(s1, s - 2, half).wait_send()

            for half in range(2):
                def body(cols, t, half=half):
                    y = yown[half, :, cols] + recv0[b, half, :, cols].astype(F32)
                    keep[b, half, :, cols] = y[:ROWS]
                    s1[b, half, :, cols] = y[ROWS:].astype(BF16)
                tiles(body)
                hop(s1, s, half).start()

        def stage_d(s):
            b = s % 2
            x_load(s).wait()

            for half in range(2):
                hop(s1, s, half).wait_recv()

                def body(cols, t, half=half):
                    y = (keep[b, half, :, cols] + r1[s % 4, half, :, cols].astype(F32)).astype(BF16).astype(F32)
                    whole = pl.ds(pl.multiple_of(half * HALF + t * TILE, TILE), TILE)
                    out_ref[pl.ds(pl.multiple_of(s * ROWS, ROWS), ROWS), whole] = (x_v[:, whole].astype(F32) + y).astype(BF16)
                tiles(body)

        def attend(i, h):
            q = jnp.concatenate([q_ref[h, pl.ds(pl.multiple_of(d * BLOCK + i * ROWS, ROWS), ROWS), :] for d in range(TP)], axis=0)
            dims = (((1,), (1,)), ((), ()))

            def scores(j):
                return lax.dot_general(q[j * ROWS:], k_ref[h, j * BLOCK:(j + 1) * BLOCK, :], dims, preferred_element_type=F32)

            row = lax.broadcasted_iota(jnp.int32, (ROWS, BLOCK), 0) + i * ROWS
            keep_mask = lax.broadcasted_iota(jnp.int32, (ROWS, BLOCK), 1) <= row
            m = l = acc = None
            ahead = scores(0)
            for j in range(TP):
                s = ahead
                if j + 1 < TP:
                    ahead = scores(j + 1)
                top = jnp.where(keep_mask, s[:ROWS], -1e30)
                s = top if j == TP - 1 else jnp.concatenate([top, s[ROWS:]], axis=0)
                peak = jnp.max(s, axis=1, keepdims=True) * scale
                new_m = peak if j == 0 else jnp.maximum(m, peak)
                p = jnp.exp2(s * scale - new_m)
                part = p[:, 0:128]
                for c in range(1, BLOCK // 128):
                    part = part + p[:, c * 128:(c + 1) * 128]
                pv = jnp.dot(p.astype(BF16), v_ref[h, j * BLOCK:(j + 1) * BLOCK, :], preferred_element_type=F32)
                if j == 0:
                    l, acc = part, pv
                else:
                    alpha = jnp.exp2(m - new_m)
                    l = l * alpha + part
                    acc = acc * alpha + pv
                total = jnp.sum(l[:ROWS], axis=1, keepdims=True)
                o_v[i, j * ROWS:(j + 1) * ROWS, pl.ds(pl.multiple_of(h * HEAD_DIM, HEAD_DIM), HEAD_DIM)] = (
                    acc[:ROWS] / total).astype(BF16)
                if j + 1 < TP:
                    m, l, acc = new_m[ROWS:], l[ROWS:], acc[ROWS:]

        def substep(s):
            @pl.when((s >= 3) & (s < STEPS + 3))
            def _():
                stage_d(s - 3)

            @pl.when((s >= 2) & (s < STEPS + 2))
            def _():
                x_load(s - 2).start()

            @pl.when((s >= 1) & (s <= STEPS))
            def _():
                stage_c(s - 1)

            @pl.when((s >= 0) & (s < STEPS))
            def _():
                stage_b(s)

        def step(i, carry):
            def head(h, z):
                @pl.when(i < STEPS)
                def _():
                    attend(i, h)

                    @pl.when(h == HEADS - 1)
                    def _():
                        for half in range(2):
                            for n in range(2):
                                o_part(o_v, i, half, n).start()

                @pl.when((i >= LAG) & ((h == 1) | (h == HEADS - 1)))
                def _():
                    substep(2 * (i - LAG) + h // (HEADS - 1) - 1)
                return z

            lax.fori_loop(0, HEADS, head, 0)
            return carry

        lax.fori_loop(0, LAG + STEPS // 2 + 2, step, 0)
        to_sib(ysend, STEPS - 1).wait_send()
        for s in (STEPS - 2, STEPS - 1):
            for half in range(2):
                hop(s1, s, half).wait_send()
        for s in range(STEPS):
            for half in range(2):
                for n in range(2):
                    o_part(o_v, s, half, n).wait_send()

    pl.run_scoped(attend_phase,
                  pltpu.VMEM((2, COLS, HALF), BF16),
                  pltpu.VMEM((STEPS, BLOCK, COLS), BF16),
                  pltpu.VMEM((SEQ, 128), F32),
                  pltpu.VMEM((2, 2 * ROWS, HALF), BF16),
                  pltpu.VMEM((2, 2 * ROWS, HALF), F32),
                  pltpu.VMEM((2, 2, ROWS, HALF), BF16),
                  pltpu.VMEM((2, 2, ROWS, HALF), F32),
                  pltpu.VMEM((ROWS, WIDTH), BF16))
    for p in range(PIECES):
        own(p, 0, XN).wait_send()
        own(p, 1, YN).wait_send()
        own(p, 2, SIB).wait_send()
        for f in forwards(p):
            relay(*f).wait_send()
        relay(DG, p, 6, SDG, SIB).wait_send()
    pair().wait_send()
    for k in (XN, YN, DG):
        share(k).wait_send()
    for half in range(2):
        for c in range(WO_PARTS):
            wo_part(c, half).wait_send()


def block_call(x, an, wq, wk, wv, qg, kg, wo, table):
    any_spec = pl.BlockSpec(memory_space=pl.ANY)
    vmem_spec = pl.BlockSpec(memory_space=pltpu.VMEM)
    dma = pltpu.SemaphoreType.DMA
    return pl.pallas_call(
        block_kernel,
        out_shape=[pltpu.VMEM((BLOCK, WIDTH), BF16),
                   pltpu.VMEM((HEADS, SEQ, HEAD_DIM), BF16),
                   pltpu.VMEM((HEADS, SEQ, HEAD_DIM), BF16),
                   jax.ShapeDtypeStruct((TP, BLOCK, WIDTH), BF16)],
        in_specs=[any_spec, vmem_spec, any_spec, any_spec, any_spec, vmem_spec, vmem_spec, any_spec, any_spec],
        out_specs=[vmem_spec] * 3 + [any_spec],
        scratch_shapes=[
            pltpu.VMEM((HEADS, SEQ, HEAD_DIM), BF16),
            pltpu.VMEM((64, 128), F32),
            pltpu.VMEM((64, 128), F32),
            pltpu.VMEM((TP // 2, 64, 128), F32),
            pltpu.VMEM((2, COLS, HALF), BF16),
            pltpu.VMEM((2, STEPS, 2, 2 * ROWS, COLS), BF16),
            pltpu.VMEM((2, 2, 2 * ROWS, HALF), BF16),
            pltpu.VMEM((4, 2, ROWS, HALF), BF16),
            dma((3,)), dma((2,)), dma((2, 2)), dma((7, PIECES)), dma((7, PIECES)), dma((4,)), dma((4,)),
            dma((2, WO_PARTS)), dma((2, WO_PARTS)), dma((2,)), dma(()),
            dma((2, STEPS, 2)), dma((2, STEPS, 2)), dma(()),
            dma(()), dma((2,)), dma((2, 2)), dma((4, 2)),
        ],
        compiler_params=pltpu.CompilerParams(collective_id=0, has_side_effects=True, vmem_limit_bytes=48 * 2**20),
        name="block",
    )(x, an, wq, wk, wv, qg, kg, wo, table)


def write_out(*refs):
    srcs, dsts, sems = refs[:3], refs[3:6], refs[6]
    parts = 4
    copies = []
    for n, (src, dst) in enumerate(zip(srcs, dsts)):
        size = src.shape[-2] // parts
        for p in range(parts):
            at = (slice(None),) * (len(src.shape) - 2) + (pl.ds(p * size, size),)
            copies.append(pltpu.make_async_copy(src.at[at], dst.at[at], sems.at[n, p]))
    for c in copies:
        c.start()
    for c in copies:
        c.wait()


def write_out_call(*arrays):
    return pl.pallas_call(
        write_out,
        out_shape=[jax.ShapeDtypeStruct(a.shape, a.dtype) for a in arrays],
        in_specs=[pl.BlockSpec(memory_space=pltpu.VMEM)] * 3,
        out_specs=[pl.BlockSpec(memory_space=pl.ANY)] * 3,
        scratch_shapes=[pltpu.SemaphoreType.DMA((3, 4))],
        compiler_params=pltpu.CompilerParams(vmem_limit_bytes=2**20),
        name="write_out",
    )(*[pltpu.with_memory_space_constraint(a, pltpu.VMEM) for a in arrays])


def rope_table():
    half = HEAD_DIM // 2
    freq = (10000.0 ** (-np.arange(half, dtype=np.float64) * (2.0 / HEAD_DIM))).astype(np.float32)
    angle = (np.arange(SEQ, dtype=np.float32)[:, None] * freq[None, :]).astype(np.float64)
    return np.concatenate([np.cos(angle), np.sin(angle)], axis=1).astype(np.float32)


def solution(mesh):
    table = rope_table()

    def local_block(x_local, attn_gain, wq, wk, wv, q_gain, k_gain, wo):
        out, k, v, _ = block_call(x_local[0], attn_gain[None], wq, wk, wv, q_gain, k_gain, wo, jnp.asarray(table))
        out, k, v = write_out_call(out, k, v)
        k_cache = jnp.transpose(k, (1, 0, 2))[None]
        v_cache = jnp.transpose(v, (1, 0, 2))[None]
        return out[None], k_cache, v_cache

    seq_spec = P("dp", "tp", None)
    head_spec = P("dp", None, "tp", None)
    col_spec = P(None, "tp")
    return jax.shard_map(local_block, mesh=mesh,
                         in_specs=(seq_spec, P(None), col_spec, col_spec, col_spec, P("tp"), P("tp"), P("tp", None)),
                         out_specs=(seq_spec, head_spec, head_spec), check_vma=False)
```
